128 devices in a mesh: cp: 32 (over y, z, core), tp: 4 (over x).
Axes of the slice: x: 4, y: 4, z: 4, core: 2. Of those that a mesh axis runs over, the one named last changes fastest.
Arguments:
- query_rows: bfloat16 [16384, 16384], P(('cp', 'tp')), may hold values from -48 to 48
- token_keys: bfloat16 [16384, 1024], P(('cp', 'tp')), may hold values from -5 to 5
- token_values: bfloat16 [16384, 1024], P(('cp', 'tp')), may hold values from -5 to 5
- doc_lengths: int32 [16], replicated, may hold values from 1 to 2048, 16384 in all
- block_plan: int32 [32, 32], replicated, may hold values from 0 to 31, each once within a row
Outputs:
- attended: bfloat16 [16384, 16384], P(('cp', 'tp'))
The draws below stay inside these ranges and needn't reach their ends.
Inputs may be any that keep to these rules, and one draw needn't show every extreme that they name: `doc_lengths`: the documents fill all 16384 tokens; one of them holds exactly 2048. Each row of block_plan is a permutation of 0 to 31.
All inputs are finite; a program needn't handle non-finite values.
Results may differ from the reference program's by a relative error of at most 0.012.
Values may be sent and summed in bfloat16 or wider, within the bound.
No kernel may reach another device: no remote copies, remote signals or barrier semaphores. Data moves between devices by JAX's collectives and lax.ppermute only.
A program may use at most 128 MiB of HBM per device.

```python
import math
import jax
import jax.numpy as jnp
import numpy as np
from jax import lax

QUERY_HEADS_COUNT = 128
KEY_VALUE_HEADS = 8
HEAD_SIZE = 128
TOK_CP = 512
SEQUENCE_TOKENS = 16384
DOC_MOST = 2048
NDOC = 16
SUB = 16
N_CP = 32


def paired_fields(key):
    field_key = jax.random.fold_in(key, 7)
    key_sample, query_draw = jax.random.split(field_key, 2)
    key_random_stream = jnp.clip(jax.random.normal(key_sample, (SEQUENCE_TOKENS, KEY_VALUE_HEADS, HEAD_SIZE), jnp.float32), -5.0, 5.0)
    query_field = jnp.clip(jax.random.normal(query_draw, (SEQUENCE_TOKENS, QUERY_HEADS_COUNT, HEAD_SIZE), jnp.float32), -5.0, 5.0)
    return (query_field, key_random_stream)


def draw_query_rows(key, part):
    query_field, key_random_stream = paired_fields(key)
    return query_field.reshape(SEQUENCE_TOKENS, QUERY_HEADS_COUNT * HEAD_SIZE).astype(jnp.bfloat16)


def draw_token_keys(key, part):
    query_field, key_random_stream = paired_fields(key)
    return key_random_stream.reshape(SEQUENCE_TOKENS, KEY_VALUE_HEADS * HEAD_SIZE).astype(jnp.bfloat16)


def shard_levels(own_key, shape, cuts, low, top_value):
    def one(position, parts):
        heights = jax.random.uniform(jax.random.fold_in(jax.random.fold_in(own_key, 6), position), (parts,), jnp.float32, low / len(cuts), top_value / len(cuts))
        return jnp.repeat(jnp.exp(heights), shape[position] // parts).reshape((-1,) + (1,) * (len(shape) - position - 1))

    level = one(*cuts[0])
    for cut in cuts[1:]:
        level = level * one(*cut)
    return level


def split_up(count, total, most, lean):
    weights = [(1 << 20) // math.isqrt(standing ** lean) + 1 for standing in range(2, count + 1)]
    surplus, holding = total - most - (count - 1), [1] * (count - 1)
    while surplus > 0:
        free = [i for i in range(count - 1) if holding[i] < most]
        whole, remaining = sum([weights[i] for i in free]), surplus
        for i in free:
            addition = min(most - holding[i], max(1, remaining * weights[i] // whole), surplus)
            holding[i] = holding[i] + addition
            surplus = surplus - addition
    return np.array([most] + holding)


def uneven(own_key, amount, total, most, slope):
    if amount == 2:
        one = jax.random.randint(own_key, (), max(1, total - most), min(most, total - 1) + 1)
        return jnp.stack([one, total - one])
    sizes = jnp.asarray(split_up(amount, total, most, slope), jnp.int32)
    pairs = (amount - 1) // 2
    donor, taker = sizes[1:1 + 2 * pairs:2], sizes[2:2 + 2 * pairs:2]
    slack = jnp.minimum(donor - 1, most - taker)
    passed = jax.random.randint(jax.random.fold_in(own_key, 1), (pairs,), 0, 1 << 20) % (slack + 1)
    sizes = sizes.at[1:1 + 2 * pairs:2].set(donor - passed).at[2:2 + 2 * pairs:2].set(taker + passed)
    return sizes[jax.random.permutation(jax.random.fold_in(own_key, 2), amount)]


def gaussian(key, extent, width, bound, shards=(), kind=jnp.bfloat16):
    values = jax.random.normal(key, extent, jnp.float32) * width
    if len(shards) > 0:
        values = shard_levels(key, extent, shards, -0.22, 0.18) * values
    return jnp.clip(values, min=-bound, max=bound).astype(kind)


def setup_inputs(seed: int = 0) -> dict:
    keys = jax.random.split(jax.random.key(seed), 6)
    return {
        "query_rows": draw_query_rows(jax.random.fold_in(keys[5], 71), 0),
        "token_keys": draw_token_keys(jax.random.fold_in(keys[5], 71), 0),
        "token_values": gaussian(keys[2], (SEQUENCE_TOKENS, KEY_VALUE_HEADS * HEAD_SIZE), 1.0, 5.0, ((0, 128),)),
        "doc_lengths": uneven(keys[3], NDOC, SEQUENCE_TOKENS, DOC_MOST, 0).astype(jnp.int32),
        "block_plan": jax.vmap(lambda own: jax.random.permutation(own, N_CP))(jax.random.split(keys[4], N_CP)).reshape((N_CP, N_CP)).astype(jnp.int32),
    }


def scaled_frequencies(head_width):
    exponents = np.arange(0, head_width, 2) / head_width
    inverse = 1.0 / np.power(500000.0, exponents)
    wavelength = 2.0 * np.pi / inverse
    smooth = (8192.0 / wavelength - 1.0) / 3.0
    blended = (1.0 - smooth) * inverse / 8.0 + smooth * inverse
    middle = np.where(wavelength > 8192.0, inverse / 8.0, blended)
    return np.where(wavelength < 2048.0, inverse, middle)

def rotation_tables(head_width, length):
    frequencies = scaled_frequencies(head_width)
    coarse_count = (length + 127) // 128
    coarse_angle = np.arange(coarse_count)[:, None] * 128.0 * frequencies[None, :]
    fine_angle = np.arange(128)[:, None] * 1.0 * frequencies[None, :]
    return (np.cos(coarse_angle), np.sin(coarse_angle), np.cos(fine_angle), np.sin(fine_angle))

def rotation_lookup(positions):
    tables = rotation_tables(HEAD_SIZE, SEQUENCE_TOKENS)
    upper_index = positions // 128
    lower_index = positions % 128
    cosine_high = jnp.asarray(tables[0], jnp.float32)[upper_index]
    sine_high = jnp.asarray(tables[1], jnp.float32)[upper_index]
    cosine_low = jnp.asarray(tables[2], jnp.float32)[lower_index]
    sine_low = jnp.asarray(tables[3], jnp.float32)[lower_index]
    cosine_rows = cosine_high * cosine_low - sine_high * sine_low
    sine_table = sine_high * cosine_low + cosine_high * sine_low
    return (cosine_rows, sine_table)

def apply_rotary_heads(head_rows, cosine_rows, sine_table):
    half_width = head_rows.shape[-1] // 2
    first_half = head_rows[..., :half_width]
    second_half = head_rows[..., half_width:]
    cosine_rows = cosine_rows[:, None, :]
    sine_table = sine_table[:, None, :]
    return jnp.concatenate([first_half * cosine_rows - second_half * sine_table, second_half * cosine_rows + first_half * sine_table], axis=-1)

def attend_exact(query_tile, query_pos, key_window, value_window, key_pos, doc_starts):
    first_pos = lax.optimization_barrier(jnp.max(jnp.where(doc_starts[None, :] <= query_pos[:, None], doc_starts[None, :], 0), axis=1))
    scores = jnp.einsum('rghd,wgd->ghrw', query_tile.astype(jnp.float32), key_window.astype(jnp.float32), precision=lax.Precision.HIGHEST) * (1.0 / math.sqrt(HEAD_SIZE))
    allowed = (key_pos[None, :] <= query_pos[:, None]) & (key_pos[None, :] >= first_pos[:, None])
    masked = jnp.where(allowed, scores, -1e+30)
    highest = lax.optimization_barrier(jnp.max(masked, axis=3, keepdims=True))
    raised = jnp.where(allowed, jnp.exp(masked - highest), 0.0)
    totals = lax.optimization_barrier(jnp.sum(raised, axis=3))
    weights = lax.optimization_barrier(raised.astype(jnp.bfloat16))
    mixed_values = jnp.einsum('ghrw,wgd->rghd', weights.astype(jnp.float32), value_window.astype(jnp.float32), precision=lax.Precision.HIGHEST)
    return (mixed_values / jnp.transpose(totals, (2, 0, 1))[..., None]).astype(jnp.bfloat16)

def reference(query_rows, token_keys, token_values, doc_lengths, block_plan):
    positions = jnp.arange(SEQUENCE_TOKENS, dtype=jnp.int32)
    cosine_rows, sine_table = rotation_lookup(positions)
    doc_starts = (jnp.cumsum(doc_lengths) - doc_lengths).astype(jnp.int32)
    rotary_keys = apply_rotary_heads(token_keys.astype(jnp.float32).reshape(SEQUENCE_TOKENS, KEY_VALUE_HEADS, HEAD_SIZE), cosine_rows, sine_table)
    rotary_keys = lax.optimization_barrier(rotary_keys.astype(jnp.bfloat16))
    grouped_values = token_values.reshape(SEQUENCE_TOKENS, KEY_VALUE_HEADS, HEAD_SIZE)
    block_length = min(256, TOK_CP)
    window_span = DOC_MOST + block_length

    def one_block(block_index):
        block_begin = (block_index * block_length).astype(jnp.int32)
        block_pos = block_begin + jnp.arange(block_length, dtype=jnp.int32)
        block_queries = lax.dynamic_slice_in_dim(query_rows, block_begin, block_length, 0).astype(jnp.float32).reshape(block_length, QUERY_HEADS_COUNT, HEAD_SIZE)
        rotated_heads = apply_rotary_heads(block_queries, lax.dynamic_slice_in_dim(cosine_rows, block_begin, block_length, 0), lax.dynamic_slice_in_dim(sine_table, block_begin, block_length, 0))
        rotated_heads = lax.optimization_barrier(rotated_heads.astype(jnp.bfloat16)).reshape(block_length, KEY_VALUE_HEADS, QUERY_HEADS_COUNT // KEY_VALUE_HEADS, HEAD_SIZE)
        window_begin = jnp.clip(block_begin - DOC_MOST, 0, SEQUENCE_TOKENS - window_span).astype(jnp.int32)
        key_window = lax.dynamic_slice_in_dim(rotary_keys, window_begin, window_span, 0)
        value_window = lax.dynamic_slice_in_dim(grouped_values, window_begin, window_span, 0)
        key_pos = window_begin + jnp.arange(window_span, dtype=jnp.int32)
        return attend_exact(rotated_heads, block_pos, key_window, value_window, key_pos, doc_starts).reshape(block_length, QUERY_HEADS_COUNT * HEAD_SIZE)
    attention = lax.map(one_block, jnp.arange(SEQUENCE_TOKENS // block_length, dtype=jnp.int32)).reshape(SEQUENCE_TOKENS, QUERY_HEADS_COUNT * HEAD_SIZE)
    plan_by_target = jnp.transpose(block_plan).astype(jnp.int32)
    source = jnp.arange(N_CP, dtype=jnp.int32)[None, :, None] * TOK_CP + plan_by_target[:, :, None] * SUB + jnp.arange(SUB, dtype=jnp.int32)[None, None, :]
    return attention[source.reshape(-1)]
```

```python
import math
import jax, jax.numpy as jnp, numpy as np
from jax import lax
from jax.experimental import pallas as pl
from jax.experimental.pallas import tpu as pltpu
from jax.sharding import PartitionSpec as P

HD = 128
BLOCK = 512
REACH = 2048
PAD = 128
TILE = 128
KEYS = 256
BIG = float(2 ** 20)
NDOC = 16
SEQ = 16384


def scaled_frequencies(head_width):
    exponents = np.arange(0, head_width, 2) / head_width
    inverse = 1.0 / np.power(500000.0, exponents)
    wavelength = 2.0 * np.pi / inverse
    smooth = (8192.0 / wavelength - 1.0) / 3.0
    blended = (1.0 - smooth) * inverse / 8.0 + smooth * inverse
    middle = np.where(wavelength > 8192.0, inverse / 8.0, blended)
    return np.where(wavelength < 2048.0, inverse, middle)


def rotation_tables():
    f = scaled_frequencies(HD)
    coarse = np.arange(SEQ // 128)[:, None] * 128.0 * f[None, :]
    fine = np.arange(128)[:, None] * 1.0 * f[None, :]
    parts = (np.cos(coarse), np.sin(coarse), np.cos(fine), np.sin(fine))
    return np.concatenate([np.concatenate([p, p], axis=1) for p in parts], axis=0).astype(np.float32)


def attn_kernel(group, heads, doc_ref, plan_ref, at_ref, tab_ref, q_ref, k4, k3, k2, k1, k0,
                out_ref, kaug, vt, qs, inv):
    s = at_ref[0]
    lane = lax.broadcasted_iota(jnp.int32, (1, 128), 1)
    first_token = s * BLOCK
    starts = jnp.zeros((1, 128), jnp.int32)
    ends = jnp.zeros((1, 128), jnp.int32)
    bounds = []
    begin = jnp.int32(0)
    for d in range(NDOC):
        bounds.append(begin)
        end = begin + doc_ref[d]
        starts = jnp.where(lane == d, begin, starts)
        ends = jnp.where(lane == d, end, ends)
        begin = end
    starts = jnp.where(lane == NDOC, -(1 << 20), starts)

    def note(r, c):
        inv[plan_ref[s, r]] = r
        return c

    lax.fori_loop(0, 32, note, 0)
    sign = jnp.where(lane < 64, -1.0, 1.0)

    def tables(pos):
        u = jnp.maximum(pos, 0) // 128
        C = tab_ref[pl.ds(u, 1), :]
        S = tab_ref[pl.ds(u + 128, 1), :]
        c = tab_ref[pl.ds(256, 128), :]
        n = tab_ref[pl.ds(384, 128), :]
        return C * c - S * n, (S * c + C * n) * sign

    def inside(pos):
        p = pos + lax.broadcasted_iota(jnp.int32, (128, 128), 0)
        return (p >= starts) & (p < ends)

    def rotated(x, cos, sin):
        x = x.astype(jnp.float32)
        return (x * cos + pltpu.roll(x, 64, 1) * sin).astype(jnp.bfloat16)

    base = first_token - REACH
    kaug[0:PAD, 0:128] = jnp.zeros((PAD, 128), jnp.bfloat16)
    kaug[0:PAD, 128:256] = jnp.where(inside(base - PAD), 1.0, 0.0).astype(jnp.bfloat16)
    vt[:, 0:PAD] = jnp.zeros((128, PAD), jnp.bfloat16)
    for b, ref in enumerate((k4, k3, k2, k1, k0)):
        def prep(i, c, b=b, ref=ref):
            pos = base + b * BLOCK + i * 128
            at = pl.multiple_of(PAD + b * BLOCK + i * 128, 128)
            rows = pl.ds(pl.multiple_of(i * 128, 128), 128)
            cos, sin = tables(pos)
            kaug[pl.ds(at, 128), 0:128] = rotated(ref[rows, group * 128:group * 128 + 128], cos, sin)
            kaug[pl.ds(at, 128), 128:256] = jnp.where(inside(pos), 1.0, 0.0).astype(jnp.bfloat16)
            v = ref[rows, 256 + group * 128:256 + group * 128 + 128]
            vt[:, pl.ds(at, 128)] = v.T
            return c
        lax.fori_loop(0, 4, prep, 0, unroll=True)

    scale = math.log2(math.e) / math.sqrt(HD)

    def tile(t, carry):
        pos = first_token + t * TILE
        cos, sin = tables(pos)
        bias = jnp.where(inside(pos), 0.0, -BIG).astype(jnp.bfloat16)
        for h in range(heads):
            qs[h * 128:h * 128 + 128, 0:128] = rotated(q_ref[t, :, h * 128:h * 128 + 128], cos, sin)
            qs[h * 128:h * 128 + 128, 128:256] = bias
        low = jnp.int32(0)
        for d in range(NDOC):
            low = jnp.where(bounds[d] <= pos, bounds[d], low)
        count = (pos + TILE - low + KEYS - 1) // KEYS
        end = PAD + REACH + TILE + t * TILE

        def pair(hp, n):
            q = qs[pl.ds(pl.multiple_of(hp * 256, 256), 256), :]
            scores = []
            high = None
            for k in range(n):
                at = pl.multiple_of(end - KEYS * (k + 1), 128)
                sc = lax.dot_general(kaug[pl.ds(at, KEYS), :], q, (((1,), (1,)), ((), ())),
                                     preferred_element_type=jnp.float32)
                if k == 0:
                    key = lax.broadcasted_iota(jnp.int32, (KEYS, 256), 0) - (KEYS - 128)
                    tok = lax.broadcasted_iota(jnp.int32, (KEYS, 256), 1) & 127
                    sc = jnp.where(key <= tok, sc, -1e30)
                scores.append(sc)
                top = jnp.max(sc, axis=0, keepdims=True)
                high = top if high is None else jnp.maximum(high, top)
            total = None
            acc = None
            for k in range(n):
                at = pl.multiple_of(end - KEYS * (k + 1), 128)
                raised = jnp.exp2((scores[k] - high) * scale)
                part = jnp.sum(raised, axis=0, keepdims=True)
                total = part if total is None else total + part
                mixed = lax.dot_general(vt[:, pl.ds(at, KEYS)], raised.astype(jnp.bfloat16),
                                        (((1,), (0,)), ((), ())), preferred_element_type=jnp.float32)
                acc = mixed if acc is None else acc + mixed
            o = (acc / total).T.astype(jnp.bfloat16)
            for a in range(2):
                col = pl.multiple_of(hp * 256 + a * 128, 128)
                for p in range(8):
                    out_ref[inv[t * 8 + p], :, pl.ds(col, 128)] = o[a * 128 + p * 16:a * 128 + p * 16 + 16]

        for n in range(1, 10):
            @pl.when(count == n)
            def _(n=n):
                def two(i, c):
                    pair(i, n)
                    return c
                lax.fori_loop(0, heads // 2, two, 0, unroll=UNROLL)
        return carry

    lax.fori_loop(0, BLOCK // TILE, tile, 0)

UNROLL = 2

def attn_call(group, heads, docs, plan, at, tab, q, kv):
    smem = pl.BlockSpec(memory_space=pltpu.SMEM)
    vmem = pl.BlockSpec(memory_space=pltpu.VMEM)
    return pl.pallas_call(
        lambda *r: attn_kernel(group, heads, *r),
        out_shape=jax.ShapeDtypeStruct((32, 16, heads * 128), jnp.bfloat16),
        in_specs=[smem, smem, smem] + [vmem] * 7,
        out_specs=vmem,
        scratch_shapes=[
            pltpu.VMEM((PAD + REACH + BLOCK, 256), jnp.bfloat16),
            pltpu.VMEM((128, PAD + REACH + BLOCK), jnp.bfloat16),
            pltpu.VMEM((heads * 128, 256), jnp.bfloat16),
            pltpu.SMEM((32,), jnp.int32),
        ],
        compiler_params=pltpu.CompilerParams(vmem_limit_bytes=48 << 20),
        name="attend",
    )(docs, plan, at, tab, q, *kv)


AXES = ("y", "z", "core", "x")
CHUNKS = 2


def shift_blocks(a, by):
    def seat(b):
        return b % 8 * 4 + b // 8

    pairs = [(seat(b), seat(b + by)) for b in range(32 - by)]
    return lax.ppermute(a, ("z", "core", "x"), pairs)


def swap_first(a, axis):
    return lax.all_to_all(a, axis, split_axis=0, concat_axis=0, tiled=True)


def place_kernel(chunks, width, *refs):
    out = refs[chunks]
    sem = refs[chunks + 1]
    copies = []
    for j in range(chunks):
        for g in range(4):
            copies.append(pltpu.make_async_copy(
                refs[j].at[g], out.at[:, pl.ds(g * 4096 + j * width, width)], sem.at[j * 4 + g]))
    for c in copies:
        c.start()
    for c in copies:
        c.wait()


def place(parts, width):
    n = len(parts)
    return pl.pallas_call(
        lambda *r: place_kernel(n, width, *r),
        out_shape=jax.ShapeDtypeStruct((128, 16384), jnp.bfloat16),
        in_specs=[pl.BlockSpec(memory_space=pl.ANY)] * n,
        out_specs=pl.BlockSpec(memory_space=pl.ANY),
        scratch_shapes=[pltpu.SemaphoreType.DMA((4 * n,))],
        name="place",
    )(*parts)


def split_kernel(chunk, width, rows, out, sem):
    copies = [
        pltpu.make_async_copy(rows.at[:, pl.ds(g * 4096 + chunk * width, width)], out.at[g], sem.at[g])
        for g in range(4)
    ]
    for c in copies:
        c.start()
    for c in copies:
        c.wait()


def split(rows, chunk, width):
    return pl.pallas_call(
        lambda *r: split_kernel(chunk, width, *r),
        out_shape=jax.ShapeDtypeStruct((4, 128, width), jnp.bfloat16),
        in_specs=[pl.BlockSpec(memory_space=pl.ANY)],
        out_specs=pl.BlockSpec(memory_space=pl.ANY),
        scratch_shapes=[pltpu.SemaphoreType.DMA((4,))],
        name="split",
    )(rows)


def on_device(query_rows, token_keys, token_values, doc_lengths, block_plan):
    block = (lax.axis_index("x") * 8 + lax.axis_index("z") * 2 + lax.axis_index("core")).astype(jnp.int32)
    at = block.reshape(1)
    kv = jnp.concatenate(
        [token_keys.reshape(128, 4, 256), token_values.reshape(128, 4, 256)], axis=2).transpose(1, 0, 2)
    kv = swap_first(swap_first(kv, "y"), "x").reshape(512, 512)
    r1 = shift_blocks(kv, 2)
    x1 = shift_blocks(kv, 1)
    r2 = shift_blocks(r1, 2)
    x2 = shift_blocks(r1, 1)
    tab = jnp.asarray(rotation_tables())
    done = []
    for j in range(CHUNKS):
        part = split(query_rows, j, 4096 // CHUNKS)
        part = swap_first(swap_first(part, "y"), "x")
        o = attn_call(j * 2 // CHUNKS, 32 // CHUNKS, doc_lengths, block_plan, at, tab, part, (r2, x2, r1, x1, kv))
        o = swap_first(o, ("y", "z", "core"))
        done.append(o.reshape(4, 128, 4096 // CHUNKS))
    return place(done, 4096 // CHUNKS)


def solution(mesh):
    fine = jax.sharding.Mesh(mesh.devices.reshape(4, 4, 2, 4), AXES)
    rows = P(AXES, None)
    return jax.shard_map(
        on_device, mesh=fine, in_specs=(rows, rows, rows, P(), P()), out_specs=rows, check_vma=False
    )
```

```python
import functools
import math
import jax, jax.numpy as jnp, numpy as np
from jax import lax
from jax.experimental import pallas as pl
from jax.experimental.pallas import tpu as pltpu
from jax.sharding import PartitionSpec as P

HD = 128
BLOCK = 512
REACH = 2048
PAD = 128
TILE = 128
KEYS = 256
BIG = float(2 ** 20)
NDOC = 16
SEQ = 16384


def scaled_frequencies(head_width):
    exponents = np.arange(0, head_width, 2) / head_width
    inverse = 1.0 / np.power(500000.0, exponents)
    wavelength = 2.0 * np.pi / inverse
    smooth = (8192.0 / wavelength - 1.0) / 3.0
    blended = (1.0 - smooth) * inverse / 8.0 + smooth * inverse
    middle = np.where(wavelength > 8192.0, inverse / 8.0, blended)
    return np.where(wavelength < 2048.0, inverse, middle)


def rotation_tables():
    f = scaled_frequencies(HD)
    coarse = np.arange(SEQ // 128)[:, None] * 128.0 * f[None, :]
    fine = np.arange(128)[:, None] * 1.0 * f[None, :]
    parts = (np.cos(coarse), np.sin(coarse), np.cos(fine), np.sin(fine))
    return np.concatenate([np.concatenate([p, p], axis=1) for p in parts], axis=0).astype(np.float32)


def attn_kernel(heads, doc_ref, plan_ref, at_ref, tab_ref, q_ref, k4, k3, k2, k1, k0, out_ref, kaug, vt, qs, inv):
    s = pl.program_id(0) * 8 + at_ref[0]
    lane = lax.broadcasted_iota(jnp.int32, (1, 128), 1)
    first_token = s * BLOCK
    starts = jnp.zeros((1, 128), jnp.int32)
    ends = jnp.zeros((1, 128), jnp.int32)
    bounds = []
    begin = jnp.int32(0)
    for d in range(NDOC):
        bounds.append(begin)
        end = begin + doc_ref[d]
        starts = jnp.where(lane == d, begin, starts)
        ends = jnp.where(lane == d, end, ends)
        begin = end
    starts = jnp.where(lane == NDOC, -(1 << 20), starts)

    def note(r, c):
        inv[plan_ref[s, r]] = r
        return c

    lax.fori_loop(0, 32, note, 0)
    sign = jnp.where(lane < 64, -1.0, 1.0)

    def tables(pos):
        u = jnp.maximum(pos, 0) // 128
        C = tab_ref[pl.ds(u, 1), :]
        S = tab_ref[pl.ds(u + 128, 1), :]
        c = tab_ref[pl.ds(256, 128), :]
        n = tab_ref[pl.ds(384, 128), :]
        return C * c - S * n, (S * c + C * n) * sign

    def inside(pos):
        p = pos + lax.broadcasted_iota(jnp.int32, (128, 128), 0)
        return (p >= starts) & (p < ends)

    def rotated(x, cos, sin):
        x = x.astype(jnp.float32)
        return (x * cos + pltpu.roll(x, 64, 1) * sin).astype(jnp.bfloat16)

    base = first_token - REACH
    kaug[0:PAD, 0:128] = jnp.zeros((PAD, 128), jnp.bfloat16)
    kaug[0:PAD, 128:256] = jnp.where(inside(base - PAD), 1.0, 0.0).astype(jnp.bfloat16)
    vt[:, 0:PAD] = jnp.zeros((128, PAD), jnp.bfloat16)
    for b, ref in enumerate((k4, k3, k2, k1, k0)):
        for i in range(4):
            pos = base + b * BLOCK + i * 128
            at = PAD + b * BLOCK + i * 128
            cos, sin = tables(pos)
            kaug[at:at + 128, 0:128] = rotated(ref[0, 0, i, :, 0:128], cos, sin)
            kaug[at:at + 128, 128:256] = jnp.where(inside(pos), 1.0, 0.0).astype(jnp.bfloat16)
            vt[:, at:at + 128] = ref[0, 0, i, :, 128:256].T

    scale = math.log2(math.e) / math.sqrt(HD)

    def tile(t, carry):
        pos = first_token + t * TILE
        cos, sin = tables(pos)
        bias = jnp.where(inside(pos), 0.0, -BIG).astype(jnp.bfloat16)
        for h in range(heads):
            qs[h * 128:h * 128 + 128, 0:128] = rotated(q_ref[0, t, :, h * 128:h * 128 + 128], cos, sin)
            qs[h * 128:h * 128 + 128, 128:256] = bias
        low = jnp.int32(0)
        for d in range(NDOC):
            low = jnp.where(bounds[d] <= pos, bounds[d], low)
        count = (pos + TILE - low + KEYS - 1) // KEYS
        end = PAD + REACH + TILE + t * TILE

        def score(hp, k):
            at = pl.multiple_of(end - KEYS * (k + 1), 128)
            sc = lax.dot_general(kaug[pl.ds(at, KEYS), :], qs[hp * 256:hp * 256 + 256, :],
                                 (((1,), (1,)), ((), ())), preferred_element_type=jnp.float32)
            if k == 0:
                key = lax.broadcasted_iota(jnp.int32, (KEYS, 256), 0) - (KEYS - 128)
                tok = lax.broadcasted_iota(jnp.int32, (KEYS, 256), 1) & 127
                sc = jnp.where(key <= tok, sc, -1e30)
            return sc

        def mix(sc, high, k):
            at = pl.multiple_of(end - KEYS * (k + 1), 128)
            raised = jnp.exp2((sc - high) * scale)
            part = jnp.sum(raised, axis=0, keepdims=True)
            mixed = lax.dot_general(vt[:, pl.ds(at, KEYS)], raised.astype(jnp.bfloat16),
                                    (((1,), (0,)), ((), ())), preferred_element_type=jnp.float32)
            return part, mixed

        def finish(hp, acc, total):
            o = (acc / total).T.astype(jnp.bfloat16)
            for a in range(2):
                col = hp * 256 + a * 128
                for p in range(8):
                    out_ref[inv[t * 8 + p], 0, :, col:col + 128] = o[a * 128 + p * 16:a * 128 + p * 16 + 16]

        def run(n):
            pairs = range(heads // 2)
            scores = [[score(hp, k) for k in range(n)] for hp in pairs]
            sums = []
            for hp in pairs:
                tops = [jnp.max(sc, axis=0, keepdims=True) for sc in scores[hp]]
                high = functools.reduce(jnp.maximum, tops)
                got = [mix(scores[hp][k], high, k) for k in range(n)]
                sums.append([functools.reduce(jnp.add, list(g)) for g in zip(*got)])
            for hp in pairs:
                finish(hp, sums[hp][1], sums[hp][0])

        for n in range(1, 10):
            pl.when(count == n)(functools.partial(run, n))
        return carry

    lax.fori_loop(0, BLOCK // TILE, tile, 0)


def attend(heads, docs, plan, at, tab, q, kv):
    smem = pl.BlockSpec(memory_space=pltpu.SMEM)

    def back(d):
        def index(y, docs_ref, plan_ref, at_ref):
            b = jnp.maximum(y * 8 + at_ref[0] - d, 0)
            return (b % 8, b // 8, 0, 0, 0)

        return pl.BlockSpec((1, 1, 4, 128, 256), index)

    return pl.pallas_call(
        lambda *r: attn_kernel(heads, *r),
        out_shape=jax.ShapeDtypeStruct((32, 4, 16, heads * 128), jnp.bfloat16),
        grid_spec=pltpu.PrefetchScalarGridSpec(
            num_scalar_prefetch=3,
            grid=(4,),
            in_specs=[
                pl.BlockSpec((512, 128), lambda y, *_: (0, 0)),
                pl.BlockSpec((1, 4, 128, heads * 128), lambda y, *_: (y, 0, 0, 0)),
            ] + [back(d) for d in (4, 3, 2, 1, 0)],
            out_specs=pl.BlockSpec((32, 1, 16, heads * 128), lambda y, *_: (0, y, 0, 0)),
            scratch_shapes=[
                pltpu.VMEM((PAD + REACH + BLOCK, 256), jnp.bfloat16),
                pltpu.VMEM((128, PAD + REACH + BLOCK), jnp.bfloat16),
                pltpu.VMEM((heads * 128, 256), jnp.bfloat16),
                pltpu.SMEM((32,), jnp.int32),
            ],
        ),
        compiler_params=pltpu.CompilerParams(vmem_limit_bytes=48 << 20),
        name="attend",
    )(docs, plan, at, tab, q, kv, kv, kv, kv, kv)


AXES = ("y", "z", "core", "x")
CHUNKS = 2


def split_kernel(rows, *outs):
    width = 1024 // len(outs)
    for g in range(4):
        for j, out in enumerate(outs):
            out[g] = rows[:, g * 1024 + j * width:g * 1024 + (j + 1) * width]


def split(rows):
    width = 1024 // CHUNKS
    return pl.pallas_call(
        split_kernel,
        grid=(4,),
        out_shape=[jax.ShapeDtypeStruct((16, 128, width), jnp.bfloat16)] * CHUNKS,
        in_specs=[pl.BlockSpec((128, 4096), lambda g: (0, g))],
        out_specs=[pl.BlockSpec((4, 128, width), lambda g: (g, 0, 0))] * CHUNKS,
        name="split",
    )(rows)


def place_kernel(*refs):
    out = refs[-1]
    width = 1024 // CHUNKS
    for j, part in enumerate(refs[:-1]):
        for b in range(8):
            for x in range(4):
                out[b * 16:b * 16 + 16, x * 1024 + j * width:x * 1024 + (j + 1) * width] = part[0, b, x]


def place(parts):
    width = 1024 // CHUNKS
    return pl.pallas_call(
        place_kernel,
        grid=(4,),
        out_shape=jax.ShapeDtypeStruct((128, 16384), jnp.bfloat16),
        in_specs=[pl.BlockSpec((1, 8, 4, 16, width), lambda y: (y, 0, 0, 0, 0))] * CHUNKS,
        out_specs=pl.BlockSpec((128, 4096), lambda y: (0, y)),
        name="place",
    )(*parts)


def on_device(query_rows, token_keys, token_values, doc_lengths, block_plan):
    at = (lax.axis_index("z") * 2 + lax.axis_index("core")).astype(jnp.int32).reshape(1)
    kv = jnp.concatenate([token_keys.reshape(128, 8, 128), token_values.reshape(128, 8, 128)], axis=2)
    kv = jnp.repeat(kv.transpose(1, 0, 2), 2, axis=0)
    kv = lax.all_to_all(kv, ("y", "x"), split_axis=0, concat_axis=0, tiled=True)
    kv = lax.all_gather(kv.reshape(4, 4, 128, 256), ("z", "core"), axis=0)
    tab = jnp.asarray(rotation_tables())
    width = 1024 // CHUNKS
    done = []
    for part in split(query_rows):
        part = lax.all_to_all(part, ("y", "x"), split_axis=0, concat_axis=0, tiled=True)
        o = attend(8 // CHUNKS, doc_lengths, block_plan, at, tab, part.reshape(4, 4, 128, width), kv)
        o = lax.all_to_all(o.reshape(128, 16, width), AXES, split_axis=0, concat_axis=0, tiled=True)
        done.append(o.reshape(4, 8, 4, 16, width))
    return place(done)


def solution(mesh):
    fine = jax.sharding.Mesh(mesh.devices.reshape(4, 4, 2, 4), AXES)
    rows = P(AXES, None)
    return jax.shard_map(
        on_device, mesh=fine, in_specs=(rows, rows, rows, P(), P()), out_specs=rows, check_vma=False
    )
```

```python
import functools
import math
import jax, jax.numpy as jnp, numpy as np
from jax import lax
from jax.experimental import pallas as pl
from jax.experimental.pallas import tpu as pltpu
from jax.sharding import PartitionSpec as P

HD = 128
BLOCK = 512
REACH = 2048
PAD = 128
TILE = 128
KEYS = 256
BIG = float(2 ** 20)
NDOC = 16
SEQ = 16384


def scaled_frequencies(head_width):
    exponents = np.arange(0, head_width, 2) / head_width
    inverse = 1.0 / np.power(500000.0, exponents)
    wavelength = 2.0 * np.pi / inverse
    smooth = (8192.0 / wavelength - 1.0) / 3.0
    blended = (1.0 - smooth) * inverse / 8.0 + smooth * inverse
    middle = np.where(wavelength > 8192.0, inverse / 8.0, blended)
    return np.where(wavelength < 2048.0, inverse, middle)


def rotation_tables():
    f = scaled_frequencies(HD)
    coarse = np.arange(SEQ // 128)[:, None] * 128.0 * f[None, :]
    fine = np.arange(128)[:, None] * 1.0 * f[None, :]
    parts = (np.cos(coarse), np.sin(coarse), np.cos(fine), np.sin(fine))
    return np.concatenate([np.concatenate([p, p], axis=1) for p in parts], axis=0).astype(np.float32)


def attn_kernel(heads, doc_ref, plan_ref, at_ref, tab_ref, q_ref, k4, v4, k3, k2, k1, k0, out_ref, kaug, vt, qs, inv):
    s = pl.program_id(0) * 8 + at_ref[0]
    lane = lax.broadcasted_iota(jnp.int32, (1, 128), 1)
    first_token = s * BLOCK
    starts = jnp.zeros((1, 128), jnp.int32)
    ends = jnp.zeros((1, 128), jnp.int32)
    bounds = []
    begin = jnp.int32(0)
    for d in range(NDOC):
        bounds.append(begin)
        end = begin + doc_ref[d]
        starts = jnp.where(lane == d, begin, starts)
        ends = jnp.where(lane == d, end, ends)
        begin = end
    starts = jnp.where(lane == NDOC, -(1 << 20), starts)

    def note(r, c):
        inv[plan_ref[s, r]] = r
        return c

    lax.fori_loop(0, 32, note, 0)
    sign = jnp.where(lane < 64, -1.0, 1.0)

    def tables(pos):
        u = jnp.maximum(pos, 0) // 128
        C = tab_ref[pl.ds(u, 1), :]
        S = tab_ref[pl.ds(u + 128, 1), :]
        c = tab_ref[pl.ds(256, 128), :]
        n = tab_ref[pl.ds(384, 128), :]
        return C * c - S * n, (S * c + C * n) * sign

    def inside(pos):
        p = pos + lax.broadcasted_iota(jnp.int32, (128, 128), 0)
        return (p >= starts) & (p < ends)

    def rotated(x, cos, sin):
        x = x.astype(jnp.float32)
        return (x * cos + pltpu.roll(x, 64, 1) * sin).astype(jnp.bfloat16)

    base = first_token - REACH
    kaug[0:PAD, 0:128] = jnp.zeros((PAD, 128), jnp.bfloat16)
    kaug[0:PAD, 128:256] = jnp.where(inside(base - PAD), 1.0, 0.0).astype(jnp.bfloat16)
    vt[:, 0:PAD] = jnp.zeros((128, PAD), jnp.bfloat16)
    for b, (kr, vr, vc) in enumerate(
            ((k4, v4, 0), (k3, k3, 128), (k2, k2, 128), (k1, k1, 128), (k0, k0, 128))):
        for i in range(4):
            pos = base + b * BLOCK + i * 128
            at = PAD + b * BLOCK + i * 128
            cos, sin = tables(pos)
            kaug[at:at + 128, 0:128] = rotated(kr[0, i, :, 0:128], cos, sin)
            kaug[at:at + 128, 128:256] = jnp.where(inside(pos), 1.0, 0.0).astype(jnp.bfloat16)
            vt[:, at:at + 128] = vr[0, i, :, vc:vc + 128].T

    scale = math.log2(math.e) / math.sqrt(HD)

    def tile(t, carry):
        pos = first_token + t * TILE
        cos, sin = tables(pos)
        bias = jnp.where(inside(pos), 0.0, -BIG).astype(jnp.bfloat16)
        for h in range(heads):
            qs[h * 128:h * 128 + 128, 0:128] = rotated(q_ref[0, t, :, h * 128:h * 128 + 128], cos, sin)
            qs[h * 128:h * 128 + 128, 128:256] = bias
        low = jnp.int32(0)
        for d in range(NDOC):
            low = jnp.where(bounds[d] <= pos, bounds[d], low)
        count = (pos + TILE - low + KEYS - 1) // KEYS
        end = PAD + REACH + TILE + t * TILE

        def score(hp, k):
            at = pl.multiple_of(end - KEYS * (k + 1), 128)
            sc = lax.dot_general(kaug[pl.ds(at, KEYS), :], qs[hp * 256:hp * 256 + 256, :],
                                 (((1,), (1,)), ((), ())), preferred_element_type=jnp.float32)
            if k == 0:
                key = lax.broadcasted_iota(jnp.int32, (KEYS, 256), 0) - (KEYS - 128)
                tok = lax.broadcasted_iota(jnp.int32, (KEYS, 256), 1) & 127
                sc = jnp.where(key <= tok, sc, -1e30)
            return sc

        def mix(sc, high, k):
            at = pl.multiple_of(end - KEYS * (k + 1), 128)
            raised = jnp.exp2((sc - high) * scale)
            part = jnp.sum(raised, axis=0, keepdims=True)
            mixed = lax.dot_general(vt[:, pl.ds(at, KEYS)], raised.astype(jnp.bfloat16),
                                    (((1,), (0,)), ((), ())), preferred_element_type=jnp.float32)
            return part, mixed

        def finish(hp, acc, total):
            o = (acc / total).T.astype(jnp.bfloat16)
            for a in range(2):
                col = hp * 256 + a * 128
                for p in range(8):
                    out_ref[inv[t * 8 + p], 0, :, col:col + 128] = o[a * 128 + p * 16:a * 128 + p * 16 + 16]

        def run(n):
            pairs = range(heads // 2)
            scores = [[score(hp, k) for k in range(n)] for hp in pairs]
            sums = []
            for hp in pairs:
                tops = [jnp.max(sc, axis=0, keepdims=True) for sc in scores[hp]]
                high = functools.reduce(jnp.maximum, tops)
                got = [mix(scores[hp][k], high, k) for k in range(n)]
                sums.append([functools.reduce(jnp.add, list(g)) for g in zip(*got)])
            for hp in pairs:
                finish(hp, sums[hp][1], sums[hp][0])

        for n in range(1, 10):
            pl.when(count == n)(functools.partial(run, n))
        return carry

    lax.fori_loop(0, BLOCK // TILE, tile, 0)


def attend(heads, docs, plan, at, tab, q, kv):
    smem = pl.BlockSpec(memory_space=pltpu.SMEM)

    def back(d, width):
        def index(y, docs_ref, plan_ref, at_ref):
            return (jnp.maximum(jnp.where(at_ref[0] < d, y - 1, y), 0), 0, 0, 0)

        return pl.BlockSpec((1, 4, 128, width), index)

    work = 16 * heads * 128 * 9 * 256 * 2 * 512
    return pl.pallas_call(
        lambda *r: attn_kernel(heads, *r),
        out_shape=jax.ShapeDtypeStruct((32, 4, 16, heads * 128), jnp.bfloat16),
        grid_spec=pltpu.PrefetchScalarGridSpec(
            num_scalar_prefetch=3,
            grid=(4,),
            in_specs=[
                pl.BlockSpec((512, 128), lambda y, *_: (0, 0)),
                pl.BlockSpec((1, 4, 128, heads * 128), lambda y, *_: (y, 0, 0, 0)),
            ] + [back(4, 128), back(4, 128), back(3, 256), back(2, 256), back(1, 256), back(0, 256)],
            out_specs=pl.BlockSpec((32, 1, 16, heads * 128), lambda y, *_: (0, y, 0, 0)),
            scratch_shapes=[
                pltpu.VMEM((PAD + REACH + BLOCK, 256), jnp.bfloat16),
                pltpu.VMEM((128, PAD + REACH + BLOCK), jnp.bfloat16),
                pltpu.VMEM((heads * 128, 256), jnp.bfloat16),
                pltpu.SMEM((32,), jnp.int32),
            ],
        ),
        compiler_params=pltpu.CompilerParams(vmem_limit_bytes=48 << 20),
        cost_estimate=pl.CostEstimate(flops=work, bytes_accessed=16 << 20, transcendentals=0),
        name="attend",
    )(docs, plan, at, tab, q, *kv)


AXES = ("y", "z", "core", "x")
CHUNKS = 2


def pack_kernel(keys, values, out):
    for g in range(8):
        for twin in range(2):
            out[2 * g + twin, :, 0:128] = keys[:, g * 128:g * 128 + 128]
            out[2 * g + twin, :, 128:256] = values[:, g * 128:g * 128 + 128]


def pack(keys, values):
    return pl.pallas_call(
        pack_kernel,
        out_shape=jax.ShapeDtypeStruct((16, 128, 256), jnp.bfloat16),
        name="pack",
    )(keys, values)


def split_kernel(rows, *outs):
    width = 1024 // len(outs)
    for g in range(4):
        for j, out in enumerate(outs):
            out[g] = rows[:, g * 1024 + j * width:g * 1024 + (j + 1) * width]


def split(rows):
    width = 1024 // CHUNKS
    return pl.pallas_call(
        split_kernel,
        grid=(4,),
        out_shape=[jax.ShapeDtypeStruct((16, 128, width), jnp.bfloat16)] * CHUNKS,
        in_specs=[pl.BlockSpec((128, 4096), lambda g: (0, g))],
        out_specs=[pl.BlockSpec((4, 128, width), lambda g: (g, 0, 0))] * CHUNKS,
        cost_estimate=pl.CostEstimate(flops=2 << 30, bytes_accessed=8 << 20, transcendentals=0),
        name="split",
    )(rows)


def place_kernel(*refs):
    out = refs[-1]
    width = 1024 // CHUNKS
    for j, part in enumerate(refs[:-1]):
        for b in range(8):
            for x in range(4):
                out[b * 16:b * 16 + 16, x * 1024 + j * width:x * 1024 + (j + 1) * width] = part[0, b, x]


def place(parts):
    width = 1024 // CHUNKS
    return pl.pallas_call(
        place_kernel,
        grid=(4,),
        out_shape=jax.ShapeDtypeStruct((128, 16384), jnp.bfloat16),
        in_specs=[pl.BlockSpec((1, 8, 4, 16, width), lambda y: (y, 0, 0, 0, 0))] * CHUNKS,
        out_specs=pl.BlockSpec((128, 4096), lambda y: (0, y)),
        name="place",
    )(*parts)


def ring(a, by):
    return lax.ppermute(a, "z", [(i, (i + by) % 4) for i in range(4)])


def swap(a):
    return lax.ppermute(a, "core", [(0, 1), (1, 0)])


def on_device(query_rows, token_keys, token_values, doc_lengths, block_plan):
    at = (lax.axis_index("z") * 2 + lax.axis_index("core")).astype(jnp.int32).reshape(1)
    core = lax.axis_index("core")
    kv = pack(token_keys, token_values)
    own = lax.all_to_all(kv, ("y", "x"), split_axis=0, concat_axis=0, tiled=True).reshape(4, 4, 128, 256)
    parts = split(query_rows)
    own, *parts = lax.optimization_barrier((own, *parts))
    near = ring(own, 1)
    left_values = ring(own[..., 128:], -1)
    far_keys = ring(near[..., :128], 1)
    far_values = ring(left_values, -1)
    first = swap(jnp.where(core == 0, own, near))
    third = swap(jnp.where(core == 0, near, jnp.concatenate([far_keys, far_values], axis=-1)))
    kv = (far_keys, far_values, third, near, first, own)
    tab = jnp.asarray(rotation_tables())
    width = 1024 // CHUNKS
    done = []
    for part in parts:
        part = lax.all_to_all(part, ("y", "x"), split_axis=0, concat_axis=0, tiled=True)
        o = attend(8 // CHUNKS, doc_lengths, block_plan, at, tab, part.reshape(4, 4, 128, width), kv)
        o = lax.all_to_all(o.reshape(128, 16, width), AXES, split_axis=0, concat_axis=0, tiled=True)
        done.append(o.reshape(4, 8, 4, 16, width))
    return place(done)


def solution(mesh):
    fine = jax.sharding.Mesh(mesh.devices.reshape(4, 4, 2, 4), AXES)
    rows = P(AXES, None)
    return jax.shard_map(
        on_device, mesh=fine, in_specs=(rows, rows, rows, P(), P()), out_specs=rows, check_vma=False
    )
```

```python
import functools
import math
import jax, jax.numpy as jnp, numpy as np
from jax import lax
from jax.experimental import pallas as pl
from jax.experimental.pallas import tpu as pltpu
from jax.sharding import PartitionSpec as P

HD = 128
BLOCK = 512
REACH = 2048
TILE = 256
KEYS = 256
BIG = float(2 ** 20)
NDOC = 16
SEQ = 16384


def scaled_frequencies(head_width):
    exponents = np.arange(0, head_width, 2) / head_width
    inverse = 1.0 / np.power(500000.0, exponents)
    wavelength = 2.0 * np.pi / inverse
    smooth = (8192.0 / wavelength - 1.0) / 3.0
    blended = (1.0 - smooth) * inverse / 8.0 + smooth * inverse
    middle = np.where(wavelength > 8192.0, inverse / 8.0, blended)
    return np.where(wavelength < 2048.0, inverse, middle)


def rotation_tables():
    f = scaled_frequencies(HD)
    coarse = np.arange(SEQ // 128)[:, None] * 128.0 * f[None, :]
    fine = np.arange(128)[:, None] * 1.0 * f[None, :]
    parts = (np.cos(coarse), np.sin(coarse), np.cos(fine), np.sin(fine))
    return np.concatenate([np.concatenate([p, p], axis=1) for p in parts], axis=0).astype(np.float32)


def tables(tab, u):
    sign = jnp.where(lax.broadcasted_iota(jnp.int32, (1, 128), 1) < 64, -1.0, 1.0)
    C = tab[pl.ds(u, 1), :]
    S = tab[pl.ds(u + 128, 1), :]
    c = tab[256:384, :]
    n = tab[384:512, :]
    return C * c - S * n, (S * c + C * n) * sign


def rotated(x, cos, sin):
    x = x.astype(jnp.float32)
    return (x * cos + pltpu.roll(x, 64, 1) * sin).astype(jnp.bfloat16)


def attn_kernel(heads, doc_ref, plan_ref, at_ref, q_ref, k4, v4, k3, k2, k1, k0, out_ref, kaug, vt, qs, inv):
    s = pl.program_id(0) * 8 + at_ref[0]
    lane = lax.broadcasted_iota(jnp.int32, (1, 128), 1)
    first_token = s * BLOCK
    starts = jnp.zeros((1, 128), jnp.int32)
    ends = jnp.zeros((1, 128), jnp.int32)
    bounds = []
    begin = jnp.int32(0)
    for d in range(NDOC):
        bounds.append(begin)
        end = begin + doc_ref[d]
        starts = jnp.where(lane == d, begin, starts)
        ends = jnp.where(lane == d, end, ends)
        begin = end
    starts = jnp.where(lane == NDOC, -(1 << 20), starts)

    def note(r, c):
        inv[plan_ref[s, r]] = r
        return c

    lax.fori_loop(0, 32, note, 0)
    def inside(pos):
        p = pos + lax.broadcasted_iota(jnp.int32, (128, 128), 0)
        return (p >= starts) & (p < ends)

    base = first_token - REACH
    scale = math.log2(math.e) / math.sqrt(HD)
    spans = []
    for t in range(BLOCK // TILE):
        pos = first_token + t * TILE
        low = jnp.int32(0)
        for d in range(NDOC):
            low = jnp.where(bounds[d] <= pos, bounds[d], low)
        need = (pos + TILE - low + KEYS - 1) // KEYS
        span = jnp.int32(SPANS[-1])
        for n in reversed(SPANS[:-1]):
            span = jnp.where(need <= n, n, span)
        spans.append(span)
    lowest = functools.reduce(
        jnp.minimum, [REACH + TILE * (t + 1) - KEYS * spans[t] for t in range(BLOCK // TILE)])

    vt[128:144, :] = jnp.ones((16, REACH + BLOCK), jnp.bfloat16)
    for b, (kr, vr, vc) in enumerate(
            ((k4, v4, 0), (k3, k3, 128), (k2, k2, 128), (k1, k1, 128), (k0, k0, 128))):
        @pl.when((b + 1) * BLOCK > lowest)
        def _(b=b, kr=kr, vr=vr, vc=vc):
            for i in range(4):
                pos = base + b * BLOCK + i * 128
                at = b * BLOCK + i * 128
                kaug[at:at + 128, 0:128] = kr[0, i, :, 0:128]
                kaug[at:at + 128, 128:256] = jnp.where(inside(pos), 1.0, 0.0).astype(jnp.bfloat16)
                vt[0:128, at:at + 128] = vr[0, i, :, vc:vc + 128]

    def score(start, h, n):
        sc = lax.dot_general(kaug[pl.ds(start, KEYS * n), :], qs[h * TILE:h * TILE + TILE, :],
                             (((1,), (1,)), ((), ())), preferred_element_type=jnp.float32)
        key = lax.broadcasted_iota(jnp.int32, (KEYS, TILE), 0)
        tok = lax.broadcasted_iota(jnp.int32, (KEYS, TILE), 1)
        parts = [sc[KEYS * k:KEYS * k + KEYS] for k in range(n)]
        parts[-1] = jnp.where(key <= tok, parts[-1], -1e30)
        high = functools.reduce(jnp.maximum, [jnp.max(x, axis=0, keepdims=True) for x in parts])
        return parts, high

    def mix(start, t, h, n, parts, high):
        p = [jnp.exp2((x - high) * scale).astype(jnp.bfloat16) for x in parts]
        got = lax.dot_general(vt[:, pl.ds(start, KEYS * n)], jnp.concatenate(p, axis=0),
                              (((1,), (0,)), ((), ())), preferred_element_type=jnp.float32)
        o = (got[0:128] * (1.0 / got[128:129])).T.astype(jnp.bfloat16)
        for i in range(TILE // 16):
            out_ref[inv[t * (TILE // 16) + i], 0, :, h * 128:h * 128 + 128] = o[i * 16:i * 16 + 16]

    def tile(t, carry):
        for u in range(TILE // 128):
            pos = first_token + t * TILE + u * 128
            bias = jnp.where(inside(pos), 0.0, -BIG).astype(jnp.bfloat16)
            for h in range(heads):
                at = h * TILE + u * 128
                qs[at:at + 128, 0:128] = q_ref[0, t * (TILE // 128) + u, :, h * 128:h * 128 + 128]
                qs[at:at + 128, 128:256] = bias
        span = jnp.where(t == 0, spans[0], spans[1])

        def run(n):
            start = pl.multiple_of(REACH + TILE * (t + 1) - KEYS * n, 256)
            got = {}
            for h in range(heads + AHEAD):
                if h < heads:
                    got[h] = score(start, h, n)
                if h >= AHEAD:
                    mix(start, t, h - AHEAD, n, *got.pop(h - AHEAD))

        for n in SPANS:
            pl.when(span == n)(functools.partial(run, n))
        return carry

    lax.fori_loop(0, BLOCK // TILE, tile, 0)


AHEAD = 3
SPANS = (1, 2, 3, 4, 5, 7, 9)


def attend(heads, docs, plan, at, q, kv):
    smem = pl.BlockSpec(memory_space=pltpu.SMEM)

    def back(d, width):
        def index(y, docs_ref, plan_ref, at_ref):
            return (jnp.maximum(jnp.where(at_ref[0] < d, y - 1, y), 0), 0, 0, 0)

        return pl.BlockSpec((1, 4, 128, width), index)

    work = 16 * heads * 128 * 9 * 256 * 2 * 512
    return pl.pallas_call(
        lambda *r: attn_kernel(heads, *r),
        out_shape=jax.ShapeDtypeStruct((32, 4, 16, heads * 128), jnp.bfloat16),
        grid_spec=pltpu.PrefetchScalarGridSpec(
            num_scalar_prefetch=3,
            grid=(4,),
            in_specs=[
                pl.BlockSpec((1, 4, 128, heads * 128), lambda y, *_: (y, 0, 0, 0)),
            ] + [back(4, 128), back(4, 128), back(3, 256), back(2, 256), back(1, 256), back(0, 256)],
            out_specs=pl.BlockSpec((32, 1, 16, heads * 128), lambda y, *_: (0, y, 0, 0)),
            scratch_shapes=[
                pltpu.VMEM((REACH + BLOCK, 256), jnp.bfloat16),
                pltpu.VMEM((144, REACH + BLOCK), jnp.bfloat16),
                pltpu.VMEM((heads * TILE, 256), jnp.bfloat16),
                pltpu.SMEM((32,), jnp.int32),
            ],
        ),
        compiler_params=pltpu.CompilerParams(vmem_limit_bytes=48 << 20),
        cost_estimate=pl.CostEstimate(flops=work, bytes_accessed=16 << 20, transcendentals=0),
        name="attend",
    )(docs, plan, at, q, *kv)


AXES = ("y", "z", "core", "x")
CHUNKS = 2


def pack_kernel(seat, tab, keys, values, out):
    cos, sin = tables(tab, seat[0])
    for g in range(8):
        k = rotated(keys[:, g * 128:g * 128 + 128], cos, sin)
        v = values[:, g * 128:g * 128 + 128].T
        for twin in range(2):
            out[2 * g + twin, :, 0:128] = k
            out[2 * g + twin, :, 128:256] = v


def pack(seat, tab, keys, values):
    return pl.pallas_call(
        pack_kernel,
        out_shape=jax.ShapeDtypeStruct((16, 128, 256), jnp.bfloat16),
        in_specs=[pl.BlockSpec(memory_space=pltpu.SMEM)] + [pl.BlockSpec(memory_space=pltpu.VMEM)] * 3,
        name="pack",
    )(seat, tab, keys, values)


def split_kernel(seat, tab, rows, *outs):
    cos, sin = tables(tab, seat[0])
    count = 8 // len(outs)
    for g in range(4):
        for j, out in enumerate(outs):
            for h in range(count):
                col = g * 1024 + (j * count + h) * 128
                out[g, :, h * 128:h * 128 + 128] = rotated(rows[:, col:col + 128], cos, sin)


def split(seat, tab, rows):
    width = 1024 // CHUNKS
    return pl.pallas_call(
        split_kernel,
        grid=(4,),
        out_shape=[jax.ShapeDtypeStruct((16, 128, width), jnp.bfloat16)] * CHUNKS,
        in_specs=[
            pl.BlockSpec(memory_space=pltpu.SMEM),
            pl.BlockSpec((512, 128), lambda g: (0, 0)),
            pl.BlockSpec((128, 4096), lambda g: (0, g)),
        ],
        out_specs=[pl.BlockSpec((4, 128, width), lambda g: (g, 0, 0))] * CHUNKS,
        cost_estimate=pl.CostEstimate(flops=2 << 30, bytes_accessed=8 << 20, transcendentals=0),
        name="split",
    )(seat, tab, rows)


def place_kernel(chunk, part, *refs):
    out, sem = refs[-2:]
    width = 1024 // CHUNKS
    copies = []
    for y in range(4):
        for b in range(8):
            for x in range(4):
                copies.append(pltpu.make_async_copy(
                    part.at[y, b, x],
                    out.at[pl.ds(b * 16, 16), pl.ds((y * 4 + x) * 1024 + chunk * width, width)],
                    sem.at[len(copies)]))
    for c in copies:
        c.start()
    for c in copies:
        c.wait()


def place(chunk, part, rows):
    before = [] if rows is None else [rows]
    return pl.pallas_call(
        functools.partial(place_kernel, chunk),
        out_shape=jax.ShapeDtypeStruct((128, 16384), jnp.bfloat16),
        in_specs=[pl.BlockSpec(memory_space=pltpu.VMEM)] + [pl.BlockSpec(memory_space=pl.ANY)] * len(before),
        out_specs=pl.BlockSpec(memory_space=pl.ANY),
        scratch_shapes=[pltpu.SemaphoreType.DMA((128,))],
        input_output_aliases={1: 0} if before else {},
        name="place",
    )(part, *before)


def ring(a, by):
    return lax.ppermute(a, "z", [(i, (i + by) % 4) for i in range(4)])


def swap(a):
    return lax.ppermute(a, "core", [(0, 1), (1, 0)])


def on_device(query_rows, token_keys, token_values, doc_lengths, block_plan):
    at = (lax.axis_index("z") * 2 + lax.axis_index("core")).astype(jnp.int32).reshape(1)
    core = lax.axis_index("core")
    seat = ((lax.axis_index("y") * 8 + at[0]) * 4 + lax.axis_index("x")).astype(jnp.int32).reshape(1)
    tab = jnp.asarray(rotation_tables())
    kv = pack(seat, tab, token_keys, token_values)
    own = lax.all_to_all(kv, ("y", "x"), split_axis=0, concat_axis=0, tiled=True).reshape(4, 4, 128, 256)
    parts = split(seat, tab, query_rows)
    own, *parts = lax.optimization_barrier((own, *parts))
    near = ring(own, 1)
    left_values = ring(own[..., 128:], -1)
    far_keys = ring(near[..., :128], 1)
    far_values = ring(left_values, -1)
    first = swap(jnp.where(core == 0, own, near))
    third = swap(jnp.where(core == 0, near, jnp.concatenate([far_keys, far_values], axis=-1)))
    kv = (far_keys, far_values, third, near, first, own)
    width = 1024 // CHUNKS
    rows = None
    for j, part in enumerate(parts):
        part = lax.all_to_all(part, ("y", "x"), split_axis=0, concat_axis=0, tiled=True)
        o = attend(8 // CHUNKS, doc_lengths, block_plan, at, part.reshape(4, 4, 128, width), kv)
        o = lax.all_to_all(o.reshape(128, 16, width), AXES, split_axis=0, concat_axis=0, tiled=True)
        rows = place(j, o.reshape(4, 8, 4, 16, width), rows)
    return rows


def solution(mesh):
    fine = jax.sharding.Mesh(mesh.devices.reshape(4, 4, 2, 4), AXES)
    rows = P(AXES, None)
    return jax.shard_map(
        on_device, mesh=fine, in_specs=(rows, rows, rows, P(), P()), out_specs=rows, check_vma=False
    )
```

```python
import functools
import math
import jax, jax.numpy as jnp, numpy as np
from jax import lax
from jax.experimental import pallas as pl
from jax.experimental.pallas import tpu as pltpu
from jax.sharding import PartitionSpec as P

HD = 128
BLOCK = 512
REACH = 2048
TILE = 256
KEYS = 256
BIG = float(2 ** 20)
NDOC = 16
SEQ = 16384


def scaled_frequencies(head_width):
    exponents = np.arange(0, head_width, 2) / head_width
    inverse = 1.0 / np.power(500000.0, exponents)
    wavelength = 2.0 * np.pi / inverse
    smooth = (8192.0 / wavelength - 1.0) / 3.0
    blended = (1.0 - smooth) * inverse / 8.0 + smooth * inverse
    middle = np.where(wavelength > 8192.0, inverse / 8.0, blended)
    return np.where(wavelength < 2048.0, inverse, middle)


def rotation_tables():
    f = scaled_frequencies(HD)
    coarse = np.arange(SEQ // 128)[:, None] * 128.0 * f[None, :]
    fine = np.arange(128)[:, None] * 1.0 * f[None, :]
    parts = (np.cos(coarse), np.sin(coarse), np.cos(fine), np.sin(fine))
    return np.concatenate([np.concatenate([p, p], axis=1) for p in parts], axis=0).astype(np.float32)


def tables(tab, u):
    sign = jnp.where(lax.broadcasted_iota(jnp.int32, (1, 128), 1) < 64, -1.0, 1.0)
    C = tab[pl.ds(u, 1), :]
    S = tab[pl.ds(u + 128, 1), :]
    c = tab[256:384, :]
    n = tab[384:512, :]
    return C * c - S * n, (S * c + C * n) * sign


def rotated(x, cos, sin):
    x = x.astype(jnp.float32)
    return (x * cos + pltpu.roll(x, 64, 1) * sin).astype(jnp.bfloat16)


def attn_kernel(heads, doc_ref, plan_ref, at_ref, q_ref, k4, v4, k3, k2, k1, k0, out_ref, kaug, vt, qs, inv):
    s = pl.program_id(0) * 8 + at_ref[0]
    lane = lax.broadcasted_iota(jnp.int32, (1, 128), 1)
    first_token = s * BLOCK
    starts = jnp.zeros((1, 128), jnp.int32)
    ends = jnp.zeros((1, 128), jnp.int32)
    bounds = []
    begin = jnp.int32(0)
    for d in range(NDOC):
        bounds.append(begin)
        end = begin + doc_ref[d]
        starts = jnp.where(lane == d, begin, starts)
        ends = jnp.where(lane == d, end, ends)
        begin = end
    starts = jnp.where(lane == NDOC, -(1 << 20), starts)

    def note(r, c):
        inv[plan_ref[s, r]] = r
        return c

    lax.fori_loop(0, 32, note, 0)
    def inside(pos):
        p = pos + lax.broadcasted_iota(jnp.int32, (128, 128), 0)
        return (p >= starts) & (p < ends)

    base = first_token - REACH
    scale = math.log2(math.e) / math.sqrt(HD)
    spans = []
    for t in range(BLOCK // TILE):
        pos = first_token + t * TILE
        low = jnp.int32(0)
        for d in range(NDOC):
            low = jnp.where(bounds[d] <= pos, bounds[d], low)
        need = (pos + TILE - low + KEYS - 1) // KEYS
        span = jnp.int32(SPANS[-1])
        for n in reversed(SPANS[:-1]):
            span = jnp.where(need <= n, n, span)
        spans.append(span)
    lowest = functools.reduce(
        jnp.minimum, [REACH + TILE * (t + 1) - KEYS * spans[t] for t in range(BLOCK // TILE)])

    vt[128:144, :] = jnp.ones((16, REACH + BLOCK), jnp.bfloat16)
    for b, (kr, vr, vc) in enumerate(
            ((k4, v4, 0), (k3, k3, 128), (k2, k2, 128), (k1, k1, 128), (k0, k0, 128))):
        @pl.when((b + 1) * BLOCK > lowest)
        def _(b=b, kr=kr, vr=vr, vc=vc):
            for i in range(4):
                pos = base + b * BLOCK + i * 128
                at = b * BLOCK + i * 128
                kaug[at:at + 128, 0:128] = kr[0, i, :, 0:128]
                kaug[at:at + 128, 128:256] = jnp.where(inside(pos), 1.0, 0.0).astype(jnp.bfloat16)
                vt[0:128, at:at + 128] = vr[0, i, :, vc:vc + 128]

    def score(start, h, n):
        sc = lax.dot_general(kaug[pl.ds(start, KEYS * n), :], qs[h * TILE:h * TILE + TILE, :],
                             (((1,), (1,)), ((), ())), preferred_element_type=jnp.float32)
        key = lax.broadcasted_iota(jnp.int32, (KEYS, TILE), 0)
        tok = lax.broadcasted_iota(jnp.int32, (KEYS, TILE), 1)
        parts = [sc[KEYS * k:KEYS * k + KEYS] for k in range(n)]
        parts[-1] = jnp.where(key <= tok, parts[-1], -1e30)
        high = functools.reduce(jnp.maximum, [jnp.max(x, axis=0, keepdims=True) for x in parts])
        return parts, high

    def mix(start, t, h, n, parts, high):
        p = [jnp.exp2((x - high) * scale).astype(jnp.bfloat16) for x in parts]
        got = lax.dot_general(vt[:, pl.ds(start, KEYS * n)], jnp.concatenate(p, axis=0),
                              (((1,), (0,)), ((), ())), preferred_element_type=jnp.float32)
        o = (got[0:128] * (1.0 / got[128:129])).T.astype(jnp.bfloat16)
        for i in range(TILE // 16):
            out_ref[inv[t * (TILE // 16) + i], 0, :, h * 128:h * 128 + 128] = o[i * 16:i * 16 + 16]

    def tile(t, carry):
        for u in range(TILE // 128):
            pos = first_token + t * TILE + u * 128
            bias = jnp.where(inside(pos), 0.0, -BIG).astype(jnp.bfloat16)
            for h in range(heads):
                at = h * TILE + u * 128
                qs[at:at + 128, 0:128] = q_ref[0, t * (TILE // 128) + u, :, h * 128:h * 128 + 128]
                qs[at:at + 128, 128:256] = bias
        span = jnp.where(t == 0, spans[0], spans[1])

        def run(n):
            start = pl.multiple_of(REACH + TILE * (t + 1) - KEYS * n, 256)
            got = {}
            for h in range(heads + AHEAD):
                if h < heads:
                    got[h] = score(start, h, n)
                if h >= AHEAD:
                    mix(start, t, h - AHEAD, n, *got.pop(h - AHEAD))

        for n in SPANS:
            pl.when(span == n)(functools.partial(run, n))
        return carry

    lax.fori_loop(0, BLOCK // TILE, tile, 0)


AHEAD = 8
SPANS = (1, 2, 3, 4, 5, 7, 9)


def attend(heads, docs, plan, at, q, kv):
    smem = pl.BlockSpec(memory_space=pltpu.SMEM)

    def back(d, width):
        def index(y, docs_ref, plan_ref, at_ref):
            return (jnp.maximum(jnp.where(at_ref[0] < d, y - 1, y), 0), 0, 0, 0)

        return pl.BlockSpec((1, 4, 128, width), index)

    work = 16 * heads * 128 * 9 * 256 * 2 * 512
    return pl.pallas_call(
        lambda *r: attn_kernel(heads, *r),
        out_shape=jax.ShapeDtypeStruct((32, 4, 16, heads * 128), jnp.bfloat16),
        grid_spec=pltpu.PrefetchScalarGridSpec(
            num_scalar_prefetch=3,
            grid=(4,),
            in_specs=[
                pl.BlockSpec((1, 4, 128, heads * 128), lambda y, *_: (y, 0, 0, 0)),
            ] + [back(4, 128), back(4, 128), back(3, 256), back(2, 256), back(1, 256), back(0, 256)],
            out_specs=pl.BlockSpec((32, 1, 16, heads * 128), lambda y, *_: (0, y, 0, 0)),
            scratch_shapes=[
                pltpu.VMEM((REACH + BLOCK, 256), jnp.bfloat16),
                pltpu.VMEM((144, REACH + BLOCK), jnp.bfloat16),
                pltpu.VMEM((heads * TILE, 256), jnp.bfloat16),
                pltpu.SMEM((32,), jnp.int32),
            ],
        ),
        compiler_params=pltpu.CompilerParams(vmem_limit_bytes=48 << 20),
        cost_estimate=pl.CostEstimate(flops=work, bytes_accessed=16 << 20, transcendentals=0),
        name="attend",
    )(docs, plan, at, q, *kv)


AXES = ("y", "z", "core", "x")
SIZES = (3, 5)
FIRST = (0, 3)


def pack_kernel(seat, tab, keys, values, out):
    cos, sin = tables(tab, seat[0])
    for g in range(8):
        k = rotated(keys[:, g * 128:g * 128 + 128], cos, sin)
        v = values[:, g * 128:g * 128 + 128].T
        for twin in range(2):
            out[2 * g + twin, :, 0:128] = k
            out[2 * g + twin, :, 128:256] = v


def pack(seat, tab, keys, values):
    return pl.pallas_call(
        pack_kernel,
        out_shape=jax.ShapeDtypeStruct((16, 128, 256), jnp.bfloat16),
        in_specs=[pl.BlockSpec(memory_space=pltpu.SMEM)] + [pl.BlockSpec(memory_space=pltpu.VMEM)] * 3,
        name="pack",
    )(seat, tab, keys, values)


def split_kernel(seat, tab, rows, *outs):
    cos, sin = tables(tab, seat[0])
    for g in range(4):
        for first, size, out in zip(FIRST, SIZES, outs):
            for h in range(size):
                col = g * 1024 + (first + h) * 128
                out[g, :, h * 128:h * 128 + 128] = rotated(rows[:, col:col + 128], cos, sin)


def split(seat, tab, rows):
    return pl.pallas_call(
        split_kernel,
        grid=(4,),
        out_shape=[jax.ShapeDtypeStruct((16, 128, n * 128), jnp.bfloat16) for n in SIZES],
        in_specs=[
            pl.BlockSpec(memory_space=pltpu.SMEM),
            pl.BlockSpec((512, 128), lambda g: (0, 0)),
            pl.BlockSpec((128, 4096), lambda g: (0, g)),
        ],
        out_specs=[pl.BlockSpec((4, 128, n * 128), lambda g: (g, 0, 0)) for n in SIZES],
        cost_estimate=pl.CostEstimate(flops=2 << 30, bytes_accessed=8 << 20, transcendentals=0),
        name="split",
    )(seat, tab, rows)


def place_kernel(*refs):
    out = refs[-1]
    for first, size, part in zip(FIRST, SIZES, refs[:-1]):
        for b in range(4):
            for x in range(4):
                col = x * 1024 + first * 128
                out[b * 16:b * 16 + 16, col:col + size * 128] = part[0, b, x]


def place(parts):
    return pl.pallas_call(
        place_kernel,
        grid=(4, 2),
        out_shape=jax.ShapeDtypeStruct((128, 16384), jnp.bfloat16),
        in_specs=[pl.BlockSpec((1, 4, 4, 16, n * 128), lambda y, b: (y, b, 0, 0, 0)) for n in SIZES],
        out_specs=pl.BlockSpec((64, 4096), lambda y, b: (b, y)),
        name="place",
    )(*parts)


def ring(a, by):
    return lax.ppermute(a, "z", [(i, (i + by) % 4) for i in range(4)])


def swap(a):
    return lax.ppermute(a, "core", [(0, 1), (1, 0)])


def on_device(query_rows, token_keys, token_values, doc_lengths, block_plan):
    at = (lax.axis_index("z") * 2 + lax.axis_index("core")).astype(jnp.int32).reshape(1)
    core = lax.axis_index("core")
    seat = ((lax.axis_index("y") * 8 + at[0]) * 4 + lax.axis_index("x")).astype(jnp.int32).reshape(1)
    tab = jnp.asarray(rotation_tables())
    kv = pack(seat, tab, token_keys, token_values)
    own = lax.all_to_all(kv, ("y", "x"), split_axis=0, concat_axis=0, tiled=True).reshape(4, 4, 128, 256)
    parts = split(seat, tab, query_rows)
    own, *parts = lax.optimization_barrier((own, *parts))
    near = ring(own, 1)
    left_values = ring(own[..., 128:], -1)
    far_keys = ring(near[..., :128], 1)
    far_values = ring(left_values, -1)
    first = swap(jnp.where(core == 0, own, near))
    parts[0] = lax.all_to_all(parts[0], ("y", "x"), split_axis=0, concat_axis=0, tiled=True)
    parts[0], middle = lax.optimization_barrier((parts[0], near))
    third = swap(jnp.where(core == 0, middle, jnp.concatenate([far_keys, far_values], axis=-1)))
    kv = (far_keys, far_values, third, near, first, own)
    done = []
    for j, (size, part) in enumerate(zip(SIZES, parts)):
        if j > 0:
            part = lax.all_to_all(part, ("y", "x"), split_axis=0, concat_axis=0, tiled=True)
        o = attend(size, doc_lengths, block_plan, at, part.reshape(4, 4, 128, size * 128), kv)
        o = lax.all_to_all(o.reshape(128, 16, size * 128), AXES, split_axis=0, concat_axis=0, tiled=True)
        done.append(o.reshape(4, 8, 4, 16, size * 128))
    return place(done)


def solution(mesh):
    fine = jax.sharding.Mesh(mesh.devices.reshape(4, 4, 2, 4), AXES)
    rows = P(AXES, None)
    return jax.shard_map(
        on_device, mesh=fine, in_specs=(rows, rows, rows, P(), P()), out_specs=rows, check_vma=False
    )
```

```python
import functools
import math
import jax, jax.numpy as jnp, numpy as np
from jax import lax
from jax.experimental import pallas as pl
from jax.experimental.pallas import tpu as pltpu
from jax.sharding import PartitionSpec as P

HD = 128
BLOCK = 512
REACH = 2048
TILE = 256
KEYS = 256
BIG = float(2 ** 20)
NDOC = 16
SEQ = 16384


def scaled_frequencies(head_width):
    exponents = np.arange(0, head_width, 2) / head_width
    inverse = 1.0 / np.power(500000.0, exponents)
    wavelength = 2.0 * np.pi / inverse
    smooth = (8192.0 / wavelength - 1.0) / 3.0
    blended = (1.0 - smooth) * inverse / 8.0 + smooth * inverse
    middle = np.where(wavelength > 8192.0, inverse / 8.0, blended)
    return np.where(wavelength < 2048.0, inverse, middle)


def rotation_tables():
    f = scaled_frequencies(HD)
    coarse = np.arange(SEQ // 128)[:, None] * 128.0 * f[None, :]
    fine = np.arange(128)[:, None] * 1.0 * f[None, :]
    parts = (np.cos(coarse), np.sin(coarse), np.cos(fine), np.sin(fine))
    return np.concatenate([np.concatenate([p, p], axis=1) for p in parts], axis=0).astype(np.float32)


def tables(tab, u):
    sign = jnp.where(lax.broadcasted_iota(jnp.int32, (1, 128), 1) < 64, -1.0, 1.0)
    C = tab[pl.ds(u, 1), :]
    S = tab[pl.ds(u + 128, 1), :]
    c = tab[256:384, :]
    n = tab[384:512, :]
    return C * c - S * n, (S * c + C * n) * sign


def rotated(x, cos, sin):
    x = x.astype(jnp.float32)
    return (x * cos + pltpu.roll(x, 64, 1) * sin).astype(jnp.bfloat16)


def attn_kernel(heads, doc_ref, plan_ref, at_ref, q_ref, k4, v4, k3, k2, k1, k0, out_ref, kaug, vt, qs, inv):
    s = pl.program_id(0) * 8 + at_ref[0]
    lane = lax.broadcasted_iota(jnp.int32, (1, 128), 1)
    first_token = s * BLOCK
    starts = jnp.zeros((1, 128), jnp.int32)
    ends = jnp.zeros((1, 128), jnp.int32)
    bounds = []
    begin = jnp.int32(0)
    for d in range(NDOC):
        bounds.append(begin)
        end = begin + doc_ref[d]
        starts = jnp.where(lane == d, begin, starts)
        ends = jnp.where(lane == d, end, ends)
        begin = end
    starts = jnp.where(lane == NDOC, -(1 << 20), starts)

    for r in range(32):
        inv[plan_ref[s, r]] = r

    def inside(pos):
        p = pos + lax.broadcasted_iota(jnp.int32, (128, 128), 0)
        return (p >= starts) & (p < ends)

    base = first_token - REACH
    scale = math.log2(math.e) / math.sqrt(HD)
    spans = []
    for t in range(BLOCK // TILE):
        pos = first_token + t * TILE
        low = jnp.int32(0)
        for d in range(NDOC):
            low = jnp.where(bounds[d] <= pos, bounds[d], low)
        need = (pos + TILE - low + KEYS - 1) // KEYS
        span = jnp.int32(SPANS[-1])
        for n in reversed(SPANS[:-1]):
            span = jnp.where(need <= n, n, span)
        spans.append(span)
    lowest = functools.reduce(
        jnp.minimum, [REACH + TILE * (t + 1) - KEYS * spans[t] for t in range(BLOCK // TILE)])

    vt[128:144, :] = jnp.ones((16, REACH + BLOCK), jnp.bfloat16)
    for b, (kr, vr, vc) in enumerate(
            ((k4, v4, 0), (k3, k3, 128), (k2, k2, 128), (k1, k1, 128), (k0, k0, 128))):
        @pl.when((b + 1) * BLOCK > lowest)
        def _(b=b, kr=kr, vr=vr, vc=vc):
            for i in range(4):
                pos = base + b * BLOCK + i * 128
                at = b * BLOCK + i * 128
                kaug[at:at + 128, 0:128] = kr[0, i, :, 0:128]
                kaug[at:at + 128, 128:256] = jnp.where(inside(pos), 1.0, 0.0).astype(jnp.bfloat16)
                vt[0:128, at:at + 128] = vr[0, i, :, vc:vc + 128]

    def score(start, h, n):
        sc = lax.dot_general(kaug[pl.ds(start, KEYS * n), :], qs[h * TILE:h * TILE + TILE, :],
                             (((1,), (1,)), ((), ())), preferred_element_type=jnp.float32)
        key = lax.broadcasted_iota(jnp.int32, (KEYS, TILE), 0)
        tok = lax.broadcasted_iota(jnp.int32, (KEYS, TILE), 1)
        parts = [sc[KEYS * k:KEYS * k + KEYS] for k in range(n)]
        parts[-1] = jnp.where(key <= tok, parts[-1], -1e30)
        high = functools.reduce(jnp.maximum, [jnp.max(x, axis=0, keepdims=True) for x in parts])
        return parts, high

    def mix(start, t, h, n, parts, high):
        p = [jnp.exp2((x - high) * scale).astype(jnp.bfloat16) for x in parts]
        got = lax.dot_general(vt[:, pl.ds(start, KEYS * n)], jnp.concatenate(p, axis=0),
                              (((1,), (0,)), ((), ())), preferred_element_type=jnp.float32)
        o = (got[0:128] * (1.0 / got[128:129])).T.astype(jnp.bfloat16)
        for i in range(TILE // 16):
            out_ref[inv[t * (TILE // 16) + i], 0, :, h * 128:h * 128 + 128] = o[i * 16:i * 16 + 16]

    def tile(t, carry):
        for u in range(TILE // 128):
            pos = first_token + t * TILE + u * 128
            bias = jnp.where(inside(pos), 0.0, -BIG).astype(jnp.bfloat16)
            for h in range(heads):
                at = h * TILE + u * 128
                qs[at:at + 128, 0:128] = q_ref[0, t * (TILE // 128) + u, :, h * 128:h * 128 + 128]
                qs[at:at + 128, 128:256] = bias
        span = jnp.where(t == 0, spans[0], spans[1])

        def run(n):
            start = pl.multiple_of(REACH + TILE * (t + 1) - KEYS * n, 256)
            got = {}
            for h in range(heads + AHEAD):
                if h < heads:
                    got[h] = score(start, h, n)
                if h >= AHEAD:
                    mix(start, t, h - AHEAD, n, *got.pop(h - AHEAD))

        for n in SPANS:
            pl.when(span == n)(functools.partial(run, n))
        return carry

    lax.fori_loop(0, BLOCK // TILE, tile, 0)


AHEAD = 8
SPANS = (1, 2, 3, 4, 5, 7, 9)


def attend(heads, docs, plan, at, q, kv):
    smem = pl.BlockSpec(memory_space=pltpu.SMEM)

    def back(d, width):
        def index(y, docs_ref, plan_ref, at_ref):
            return (jnp.maximum(jnp.where(at_ref[0] < d, y - 1, y), 0), 0, 0, 0)

        return pl.BlockSpec((1, 4, 128, width), index)

    work = 16 * heads * 128 * 9 * 256 * 2 * 512
    return pl.pallas_call(
        lambda *r: attn_kernel(heads, *r),
        out_shape=jax.ShapeDtypeStruct((32, 4, 16, heads * 128), jnp.bfloat16),
        grid_spec=pltpu.PrefetchScalarGridSpec(
            num_scalar_prefetch=3,
            grid=(4,),
            in_specs=[
                pl.BlockSpec((1, 4, 128, heads * 128), lambda y, *_: (y, 0, 0, 0)),
            ] + [back(4, 128), back(4, 128), back(3, 256), back(2, 256), back(1, 256), back(0, 256)],
            out_specs=pl.BlockSpec((32, 1, 16, heads * 128), lambda y, *_: (0, y, 0, 0)),
            scratch_shapes=[
                pltpu.VMEM((REACH + BLOCK, 256), jnp.bfloat16),
                pltpu.VMEM((144, REACH + BLOCK), jnp.bfloat16),
                pltpu.VMEM((heads * TILE, 256), jnp.bfloat16),
                pltpu.SMEM((32,), jnp.int32),
            ],
        ),
        compiler_params=pltpu.CompilerParams(vmem_limit_bytes=48 << 20),
        cost_estimate=pl.CostEstimate(flops=work, bytes_accessed=16 << 20, transcendentals=0),
        name="attend",
    )(docs, plan, at, q, *kv)


AXES = ("y", "z", "core", "x")
SIZES = (4, 4)
FIRST = (0, 4)


def pack_kernel(seat, tab, keys, values, out):
    cos, sin = tables(tab, seat[0])
    for g in range(8):
        k = rotated(keys[:, g * 128:g * 128 + 128], cos, sin)
        v = values[:, g * 128:g * 128 + 128].T
        for twin in range(2):
            out[2 * g + twin, :, 0:128] = k
            out[2 * g + twin, :, 128:256] = v


def pack(seat, tab, keys, values):
    return pl.pallas_call(
        pack_kernel,
        out_shape=jax.ShapeDtypeStruct((16, 128, 256), jnp.bfloat16),
        in_specs=[pl.BlockSpec(memory_space=pltpu.SMEM)] + [pl.BlockSpec(memory_space=pltpu.VMEM)] * 3,
        name="pack",
    )(seat, tab, keys, values)


def split_kernel(seat, tab, rows, *outs):
    cos, sin = tables(tab, seat[0])
    for g in range(4):
        for first, size, out in zip(FIRST, SIZES, outs):
            for h in range(size):
                col = g * 1024 + (first + h) * 128
                out[g, :, h * 128:h * 128 + 128] = rotated(rows[:, col:col + 128], cos, sin)


def split(seat, tab, rows):
    return pl.pallas_call(
        split_kernel,
        grid=(4,),
        out_shape=[jax.ShapeDtypeStruct((16, 128, n * 128), jnp.bfloat16) for n in SIZES],
        in_specs=[
            pl.BlockSpec(memory_space=pltpu.SMEM),
            pl.BlockSpec((512, 128), lambda g: (0, 0)),
            pl.BlockSpec((128, 4096), lambda g: (0, g)),
        ],
        out_specs=[pl.BlockSpec((4, 128, n * 128), lambda g: (g, 0, 0)) for n in SIZES],
        cost_estimate=pl.CostEstimate(flops=2 << 30, bytes_accessed=8 << 20, transcendentals=0),
        name="split",
    )(seat, tab, rows)


def place_kernel(*refs):
    out = refs[-1]
    for first, size, part in zip(FIRST, SIZES, refs[:-1]):
        for b in range(8):
            for x in range(4):
                col = x * 1024 + first * 128
                out[b * 16:b * 16 + 16, col:col + size * 128] = part[0, b, x]


def place(parts):
    return pl.pallas_call(
        place_kernel,
        grid=(4,),
        out_shape=jax.ShapeDtypeStruct((128, 16384), jnp.bfloat16),
        in_specs=[pl.BlockSpec((1, 8, 4, 16, n * 128), lambda y: (y, 0, 0, 0, 0)) for n in SIZES],
        out_specs=pl.BlockSpec((128, 4096), lambda y: (0, y)),
        name="place",
    )(*parts)


def ring(a, by):
    return lax.ppermute(a, "z", [(i, (i + by) % 4) for i in range(4)])


def swap(a):
    return lax.ppermute(a, "core", [(0, 1), (1, 0)])


def on_device(query_rows, token_keys, token_values, doc_lengths, block_plan):
    at = (lax.axis_index("z") * 2 + lax.axis_index("core")).astype(jnp.int32).reshape(1)
    core = lax.axis_index("core")
    seat = ((lax.axis_index("y") * 8 + at[0]) * 4 + lax.axis_index("x")).astype(jnp.int32).reshape(1)
    tab = jnp.asarray(rotation_tables())
    kv = pack(seat, tab, token_keys, token_values)
    own = lax.all_to_all(kv, ("y", "x"), split_axis=0, concat_axis=0, tiled=True).reshape(4, 4, 128, 256)
    parts = split(seat, tab, query_rows)
    own, *parts = lax.optimization_barrier((own, *parts))
    near = ring(own, 1)
    left_values = ring(own[..., 128:], -1)
    far_keys = ring(near[..., :128], 1)
    far_values = ring(left_values, -1)
    first = swap(jnp.where(core == 0, own, near))
    parts[0] = lax.all_to_all(parts[0], ("y", "x"), split_axis=0, concat_axis=0, tiled=True)
    parts[0], middle = lax.optimization_barrier((parts[0], near))
    third = jnp.where(core == 0, middle, jnp.concatenate([far_keys, far_values], axis=-1))
    third = swap(third)
    kv = (far_keys, far_values, third, near, first, own)
    done = []
    for j, (size, part) in enumerate(zip(SIZES, parts)):
        if j > 0:
            part = lax.all_to_all(part, ("y", "x"), split_axis=0, concat_axis=0, tiled=True)
        o = attend(size, doc_lengths, block_plan, at, part.reshape(4, 4, 128, size * 128), kv)
        o = lax.all_to_all(o.reshape(128, 16, size * 128), AXES, split_axis=0, concat_axis=0, tiled=True)
        done.append(o.reshape(4, 8, 4, 16, size * 128))
    return place(done)


def solution(mesh):
    fine = jax.sharding.Mesh(mesh.devices.reshape(4, 4, 2, 4), AXES)
    rows = P(AXES, None)

    return jax.shard_map(on_device, mesh=fine, in_specs=(rows, rows, rows, P(), P()), out_specs=rows, check_vma=False)
```

```python
import functools
import math
import jax, jax.numpy as jnp, numpy as np
from jax import lax
from jax.experimental import pallas as pl
from jax.experimental.pallas import tpu as pltpu
from jax.sharding import PartitionSpec as P

HD = 128
BLOCK = 512
REACH = 2048
TILE = 256
KEYS = 256
BIG = float(2 ** 20)
NDOC = 16
SEQ = 16384


def scaled_frequencies(head_width):
    exponents = np.arange(0, head_width, 2) / head_width
    inverse = 1.0 / np.power(500000.0, exponents)
    wavelength = 2.0 * np.pi / inverse
    smooth = (8192.0 / wavelength - 1.0) / 3.0
    blended = (1.0 - smooth) * inverse / 8.0 + smooth * inverse
    middle = np.where(wavelength > 8192.0, inverse / 8.0, blended)
    return np.where(wavelength < 2048.0, inverse, middle)


def rotation_tables():
    f = scaled_frequencies(HD)
    coarse = np.arange(SEQ // 128)[:, None] * 128.0 * f[None, :]
    fine = np.arange(128)[:, None] * 1.0 * f[None, :]
    parts = (np.cos(coarse), np.sin(coarse), np.cos(fine), np.sin(fine))
    return np.concatenate([np.concatenate([p, p], axis=1) for p in parts], axis=0).astype(np.float32)


def tables(tab, u):
    sign = jnp.where(lax.broadcasted_iota(jnp.int32, (1, 128), 1) < 64, -1.0, 1.0)
    C = tab[pl.ds(u, 1), :]
    S = tab[pl.ds(u + 128, 1), :]
    c = tab[256:384, :]
    n = tab[384:512, :]
    return C * c - S * n, (S * c + C * n) * sign


def rotated(x, cos, sin):
    x = x.astype(jnp.float32)
    return (x * cos + pltpu.roll(x, 64, 1) * sin).astype(jnp.bfloat16)


def attn_kernel(heads, doc_ref, plan_ref, at_ref, q_ref, k4, v4, k3, k2, k1, k0, out_ref, kaug, vt, qs, inv):
    s = pl.program_id(0) * 8 + at_ref[0]
    lane = lax.broadcasted_iota(jnp.int32, (1, 128), 1)
    first_token = s * BLOCK
    starts = jnp.zeros((1, 128), jnp.int32)
    ends = jnp.zeros((1, 128), jnp.int32)
    bounds = []
    begin = jnp.int32(0)
    for d in range(NDOC):
        bounds.append(begin)
        end = begin + doc_ref[d]
        starts = jnp.where(lane == d, begin, starts)
        ends = jnp.where(lane == d, end, ends)
        begin = end
    starts = jnp.where(lane == NDOC, -(1 << 20), starts)

    for r in range(32):
        inv[plan_ref[s, r]] = r

    def inside(pos):
        p = pos + lax.broadcasted_iota(jnp.int32, (128, 128), 0)
        return (p >= starts) & (p < ends)

    base = first_token - REACH
    scale = math.log2(math.e) / math.sqrt(HD)
    spans = []
    for t in range(BLOCK // TILE):
        pos = first_token + t * TILE
        low = jnp.int32(0)
        for d in range(NDOC):
            low = jnp.where(bounds[d] <= pos, bounds[d], low)
        need = (pos + TILE - low + KEYS - 1) // KEYS
        span = jnp.int32(SPANS[-1])
        for n in reversed(SPANS[:-1]):
            span = jnp.where(need <= n, n, span)
        spans.append(span)
    lowest = functools.reduce(
        jnp.minimum, [REACH + TILE * (t + 1) - KEYS * spans[t] for t in range(BLOCK // TILE)])

    vt[128:144, :] = jnp.ones((16, REACH + BLOCK), jnp.bfloat16)
    for b, (kr, vr, vc) in enumerate(
            ((k4, v4, 0), (k3, k3, 128), (k2, k2, 128), (k1, k1, 128), (k0, k0, 128))):
        @pl.when((b + 1) * BLOCK > lowest)
        def _(b=b, kr=kr, vr=vr, vc=vc):
            for i in range(4):
                pos = base + b * BLOCK + i * 128
                at = b * BLOCK + i * 128
                kaug[at:at + 128, 0:128] = kr[0, i, :, 0:128]
                kaug[at:at + 128, 128:256] = jnp.where(inside(pos), 1.0, 0.0).astype(jnp.bfloat16)
                vt[0:128, at:at + 128] = vr[0, i, :, vc:vc + 128]

    def score(start, h, n):
        sc = lax.dot_general(kaug[pl.ds(start, KEYS * n), :], qs[h * TILE:h * TILE + TILE, :],
                             (((1,), (1,)), ((), ())), preferred_element_type=jnp.float32)
        key = lax.broadcasted_iota(jnp.int32, (KEYS, TILE), 0)
        tok = lax.broadcasted_iota(jnp.int32, (KEYS, TILE), 1)
        parts = [sc[KEYS * k:KEYS * k + KEYS] for k in range(n)]
        parts[-1] = jnp.where(key <= tok, parts[-1], -1e30)
        high = functools.reduce(jnp.maximum, [jnp.max(x, axis=0, keepdims=True) for x in parts])
        return parts, high

    def mix(start, t, h, n, parts, high):
        p = [jnp.exp2((x - high) * scale).astype(jnp.bfloat16) for x in parts]
        got = lax.dot_general(vt[:, pl.ds(start, KEYS * n)], jnp.concatenate(p, axis=0),
                              (((1,), (0,)), ((), ())), preferred_element_type=jnp.float32)
        o = (got[0:128] * (1.0 / got[128:129])).T.astype(jnp.bfloat16)
        for i in range(TILE // 16):
            out_ref[inv[t * (TILE // 16) + i], 0, :, h * 128:h * 128 + 128] = o[i * 16:i * 16 + 16]

    def tile(t, carry):
        for u in range(TILE // 128):
            pos = first_token + t * TILE + u * 128
            bias = jnp.where(inside(pos), 0.0, -BIG).astype(jnp.bfloat16)
            for h in range(heads):
                at = h * TILE + u * 128
                qs[at:at + 128, 0:128] = q_ref[0, t * (TILE // 128) + u, :, h * 128:h * 128 + 128]
                qs[at:at + 128, 128:256] = bias
        span = jnp.where(t == 0, spans[0], spans[1])

        def run(n):
            start = pl.multiple_of(REACH + TILE * (t + 1) - KEYS * n, 256)
            got = {}
            for h in range(heads + AHEAD):
                if h < heads:
                    got[h] = score(start, h, n)
                if h >= AHEAD:
                    mix(start, t, h - AHEAD, n, *got.pop(h - AHEAD))

        for n in SPANS:
            pl.when(span == n)(functools.partial(run, n))
        return carry

    lax.fori_loop(0, BLOCK // TILE, tile, 0)


AHEAD = 8
SPANS = (1, 2, 3, 4, 5, 7, 9)


def attend(heads, docs, plan, at, q, kv):
    smem = pl.BlockSpec(memory_space=pltpu.SMEM)

    def back(d, width):
        def index(y, docs_ref, plan_ref, at_ref):
            return (jnp.maximum(jnp.where(at_ref[0] < d, y - 1, y), 0), 0, 0, 0)

        return pl.BlockSpec((1, 4, 128, width), index)

    work = 16 * heads * 128 * 9 * 256 * 2 * 512
    return pl.pallas_call(
        lambda *r: attn_kernel(heads, *r),
        out_shape=jax.ShapeDtypeStruct((32, 4, 16, heads * 128), jnp.bfloat16),
        grid_spec=pltpu.PrefetchScalarGridSpec(
            num_scalar_prefetch=3,
            grid=(4,),
            in_specs=[
                pl.BlockSpec((1, 4, 128, heads * 128), lambda y, *_: (y, 0, 0, 0)),
            ] + [back(4, 128), back(4, 128), back(3, 256), back(2, 256), back(1, 256), back(0, 256)],
            out_specs=pl.BlockSpec((32, 1, 16, heads * 128), lambda y, *_: (0, y, 0, 0)),
            scratch_shapes=[
                pltpu.VMEM((REACH + BLOCK, 256), jnp.bfloat16),
                pltpu.VMEM((144, REACH + BLOCK), jnp.bfloat16),
                pltpu.VMEM((heads * TILE, 256), jnp.bfloat16),
                pltpu.SMEM((32,), jnp.int32),
            ],
        ),
        compiler_params=pltpu.CompilerParams(vmem_limit_bytes=VM << 20),
        cost_estimate=pl.CostEstimate(flops=work, bytes_accessed=16 << 20, transcendentals=0),
        name="attend",
    )(docs, plan, at, q, *kv)


VM = 52


AXES = ("y", "z", "core", "x")
SIZES = (4, 4)
FIRST = (0, 4)


def pack_kernel(seat, tab, keys, values, out):
    cos, sin = tables(tab, seat[0])
    for g in range(8):
        k = rotated(keys[:, g * 128:g * 128 + 128], cos, sin)
        v = values[:, g * 128:g * 128 + 128].T
        for twin in range(2):
            out[2 * g + twin, :, 0:128] = k
            out[2 * g + twin, :, 128:256] = v


def pack(seat, tab, keys, values):
    return pl.pallas_call(
        pack_kernel,
        out_shape=jax.ShapeDtypeStruct((16, 128, 256), jnp.bfloat16),
        in_specs=[pl.BlockSpec(memory_space=pltpu.SMEM)] + [pl.BlockSpec(memory_space=pltpu.VMEM)] * 3,
        name="pack",
    )(seat, tab, keys, values)


def split_kernel(seat, tab, rows, *outs):
    cos, sin = tables(tab, seat[0])
    for g in range(4):
        for first, size, out in zip(FIRST, SIZES, outs):
            for h in range(size):
                col = g * 1024 + (first + h) * 128
                out[g, :, h * 128:h * 128 + 128] = rotated(rows[:, col:col + 128], cos, sin)


def split(seat, tab, rows):
    return pl.pallas_call(
        split_kernel,
        grid=(4,),
        out_shape=[jax.ShapeDtypeStruct((16, 128, n * 128), jnp.bfloat16) for n in SIZES],
        in_specs=[
            pl.BlockSpec(memory_space=pltpu.SMEM),
            pl.BlockSpec((512, 128), lambda g: (0, 0)),
            pl.BlockSpec((128, 4096), lambda g: (0, g)),
        ],
        out_specs=[pl.BlockSpec((4, 128, n * 128), lambda g: (g, 0, 0)) for n in SIZES],
        cost_estimate=pl.CostEstimate(flops=2 << 30, bytes_accessed=8 << 20, transcendentals=0),
        name="split",
    )(seat, tab, rows)


def place_kernel(first, size, part, *refs):
    out, buf, sem = refs[-3:]
    step = pl.program_id(0)

    def copy(y, x):
        cols = pl.ds(pl.multiple_of((y * 4 + x) * 1024 + first * 128, 128), size * 128)
        return pltpu.make_async_copy(buf.at[y, x], out.at[:, cols], sem.at[y, x])

    for x in range(4):
        for b in range(8):
            buf[step, x, b * 16:b * 16 + 16, :] = part[0, b, x]
        copy(step, x).start()

    @pl.when(step == 3)
    def _():
        for y in range(4):
            for x in range(4):
                copy(y, x).wait()


def place(first, size, part, rows):
    before = [] if rows is None else [rows]
    return pl.pallas_call(
        functools.partial(place_kernel, first, size),
        grid=(4,),
        out_shape=jax.ShapeDtypeStruct((128, 16384), jnp.bfloat16),
        in_specs=[pl.BlockSpec((1, 8, 4, 16, size * 128), lambda y: (y, 0, 0, 0, 0))]
        + [pl.BlockSpec(memory_space=pl.ANY)] * len(before),
        out_specs=pl.BlockSpec(memory_space=pl.ANY),
        scratch_shapes=[
            pltpu.VMEM((4, 4, 128, size * 128), jnp.bfloat16),
            pltpu.SemaphoreType.DMA((4, 4)),
        ],
        input_output_aliases={1: 0} if before else {},
        compiler_params=pltpu.CompilerParams(vmem_limit_bytes=12 << 20),
        cost_estimate=pl.CostEstimate(flops=1 << 30, bytes_accessed=4 << 20, transcendentals=0),
        name="place",
    )(part, *before)


def ring(a, by):
    return lax.ppermute(a, "z", [(i, (i + by) % 4) for i in range(4)])


def swap(a):
    return lax.ppermute(a, "core", [(0, 1), (1, 0)])


def on_device(query_rows, token_keys, token_values, doc_lengths, block_plan):
    at = (lax.axis_index("z") * 2 + lax.axis_index("core")).astype(jnp.int32).reshape(1)
    core = lax.axis_index("core")
    seat = ((lax.axis_index("y") * 8 + at[0]) * 4 + lax.axis_index("x")).astype(jnp.int32).reshape(1)
    tab = jnp.asarray(rotation_tables())
    kv = pack(seat, tab, token_keys, token_values)
    own = lax.all_to_all(kv, ("y", "x"), split_axis=0, concat_axis=0, tiled=True).reshape(4, 4, 128, 256)
    parts = split(seat, tab, query_rows)
    own, *parts = lax.optimization_barrier((own, *parts))
    near = ring(own, 1)
    left_values = ring(own[..., 128:], -1)
    far_keys = ring(near[..., :128], 1)
    far_values = ring(left_values, -1)
    first = swap(jnp.where(core == 0, own, near))
    parts[0] = lax.all_to_all(parts[0], ("y", "x"), split_axis=0, concat_axis=0, tiled=True)
    parts[0], middle = lax.optimization_barrier((parts[0], near))
    third = jnp.where(core == 0, middle, jnp.concatenate([far_keys, far_values], axis=-1))
    third = swap(third)
    kv = (far_keys, far_values, third, near, first, own)
    rows = None
    for j, (size, part) in enumerate(zip(SIZES, parts)):
        if j > 0:
            part = lax.all_to_all(part, ("y", "x"), split_axis=0, concat_axis=0, tiled=True)
        o = attend(size, doc_lengths, block_plan, at, part.reshape(4, 4, 128, size * 128), kv)
        o = lax.all_to_all(o.reshape(128, 16, size * 128), AXES, split_axis=0, concat_axis=0, tiled=True)
        rows = place(FIRST[j], size, o.reshape(4, 8, 4, 16, size * 128), rows)
    return rows


def solution(mesh):
    fine = jax.sharding.Mesh(mesh.devices.reshape(4, 4, 2, 4), AXES)
    rows = P(AXES, None)

    return jax.shard_map(on_device, mesh=fine, in_specs=(rows, rows, rows, P(), P()), out_specs=rows, check_vma=False)
```

```python
import functools
import math
import jax, jax.numpy as jnp, numpy as np
from jax import lax
from jax.experimental import pallas as pl
from jax.experimental.pallas import tpu as pltpu
from jax.sharding import PartitionSpec as P

HD = 128
BLOCK = 512
REACH = 2048
TILE = 256
KEYS = 256
BIG = float(2 ** 20)
NDOC = 16
SEQ = 16384


def scaled_frequencies(head_width):
    exponents = np.arange(0, head_width, 2) / head_width
    inverse = 1.0 / np.power(500000.0, exponents)
    wavelength = 2.0 * np.pi / inverse
    smooth = (8192.0 / wavelength - 1.0) / 3.0
    blended = (1.0 - smooth) * inverse / 8.0 + smooth * inverse
    middle = np.where(wavelength > 8192.0, inverse / 8.0, blended)
    return np.where(wavelength < 2048.0, inverse, middle)


def rotation_tables():
    f = scaled_frequencies(HD)
    coarse = np.arange(SEQ // 128)[:, None] * 128.0 * f[None, :]
    fine = np.arange(128)[:, None] * 1.0 * f[None, :]
    parts = (np.cos(coarse), np.sin(coarse), np.cos(fine), np.sin(fine))
    return np.concatenate([np.concatenate([p, p], axis=1) for p in parts], axis=0).astype(np.float32)


def tables(tab, u):
    sign = jnp.where(lax.broadcasted_iota(jnp.int32, (1, 128), 1) < 64, -1.0, 1.0)
    C = tab[pl.ds(u, 1), :]
    S = tab[pl.ds(u + 128, 1), :]
    c = tab[256:384, :]
    n = tab[384:512, :]
    return C * c - S * n, (S * c + C * n) * sign


def rotated(x, cos, sin):
    x = x.astype(jnp.float32)
    return (x * cos + pltpu.roll(x, 64, 1) * sin).astype(jnp.bfloat16)


def attn_kernel(heads, doc_ref, plan_ref, at_ref, q_ref, k4, v4, k3, k2, k1, k0, out_ref, kaug, vt, qs, inv):
    s = pl.program_id(0) * 8 + at_ref[0]
    lane = lax.broadcasted_iota(jnp.int32, (1, 128), 1)
    first_token = s * BLOCK
    starts = jnp.zeros((1, 128), jnp.int32)
    ends = jnp.zeros((1, 128), jnp.int32)
    bounds = []
    begin = jnp.int32(0)
    for d in range(NDOC):
        bounds.append(begin)
        end = begin + doc_ref[d]
        starts = jnp.where(lane == d, begin, starts)
        ends = jnp.where(lane == d, end, ends)
        begin = end
    starts = jnp.where(lane == NDOC, -(1 << 20), starts)

    for r in range(32):
        inv[plan_ref[s, r]] = r

    def inside(pos):
        p = pos + lax.broadcasted_iota(jnp.int32, (128, 128), 0)
        return (p >= starts) & (p < ends)

    base = first_token - REACH
    scale = math.log2(math.e) / math.sqrt(HD)
    spans = []
    for t in range(BLOCK // TILE):
        pos = first_token + t * TILE
        low = jnp.int32(0)
        for d in range(NDOC):
            low = jnp.where(bounds[d] <= pos, bounds[d], low)
        need = (pos + TILE - low + KEYS - 1) // KEYS
        span = jnp.int32(SPANS[-1])
        for n in reversed(SPANS[:-1]):
            span = jnp.where(need <= n, n, span)
        spans.append(span)
    lowest = functools.reduce(
        jnp.minimum, [REACH + TILE * (t + 1) - KEYS * spans[t] for t in range(BLOCK // TILE)])

    vt[128:144, :] = jnp.ones((16, REACH + BLOCK), jnp.bfloat16)
    for b, (kr, vr, vc) in enumerate(
            ((k4, v4, 0), (k3, k3, 128), (k2, k2, 128), (k1, k1, 128), (k0, k0, 128))):
        @pl.when((b + 1) * BLOCK > lowest)
        def _(b=b, kr=kr, vr=vr, vc=vc):
            for i in range(4):
                pos = base + b * BLOCK + i * 128
                at = b * BLOCK + i * 128
                kaug[at:at + 128, 0:128] = kr[0, i, :, 0:128]
                kaug[at:at + 128, 128:256] = jnp.where(inside(pos), 1.0, 0.0).astype(jnp.bfloat16)
                vt[0:128, at:at + 128] = vr[0, i, :, vc:vc + 128]

    def score(start, h, n):
        sc = lax.dot_general(kaug[pl.ds(start, KEYS * n), :], qs[h * TILE:h * TILE + TILE, :],
                             (((1,), (1,)), ((), ())), preferred_element_type=jnp.float32)
        key = lax.broadcasted_iota(jnp.int32, (KEYS, TILE), 0)
        tok = lax.broadcasted_iota(jnp.int32, (KEYS, TILE), 1)
        parts = [sc[KEYS * k:KEYS * k + KEYS] for k in range(n)]
        parts[-1] = jnp.where(key <= tok, parts[-1], -1e30)
        high = functools.reduce(jnp.maximum, [jnp.max(x, axis=0, keepdims=True) for x in parts])
        return parts, high

    def mix(start, t, h, n, parts, high):
        p = [jnp.exp2((x - high) * scale).astype(jnp.bfloat16) for x in parts]
        got = lax.dot_general(vt[:, pl.ds(start, KEYS * n)], jnp.concatenate(p, axis=0),
                              (((1,), (0,)), ((), ())), preferred_element_type=jnp.float32)
        o = (got[0:128] * (1.0 / got[128:129])).T.astype(jnp.bfloat16)
        for i in range(TILE // 16):
            out_ref[inv[t * (TILE // 16) + i], 0, :, h * 128:h * 128 + 128] = o[i * 16:i * 16 + 16]

    def tile(t, carry):
        for u in range(TILE // 128):
            pos = first_token + t * TILE + u * 128
            bias = jnp.where(inside(pos), 0.0, -BIG).astype(jnp.bfloat16)
            for h in range(heads):
                at = h * TILE + u * 128
                qs[at:at + 128, 0:128] = q_ref[0, t * (TILE // 128) + u, :, h * 128:h * 128 + 128]
                qs[at:at + 128, 128:256] = bias
        span = jnp.where(t == 0, spans[0], spans[1])

        def run(n):
            start = pl.multiple_of(REACH + TILE * (t + 1) - KEYS * n, 256)
            got = {}
            for h in range(heads + AHEAD):
                if h < heads:
                    got[h] = score(start, h, n)
                if h >= AHEAD:
                    mix(start, t, h - AHEAD, n, *got.pop(h - AHEAD))

        for n in SPANS:
            pl.when(span == n)(functools.partial(run, n))
        return carry

    lax.fori_loop(0, BLOCK // TILE, tile, 0)


AHEAD = 8
SPANS = (1, 2, 3, 4, 5, 7, 9)


def attend(heads, docs, plan, at, q, kv):
    smem = pl.BlockSpec(memory_space=pltpu.SMEM)

    def back(d, width):
        def index(y, docs_ref, plan_ref, at_ref):
            return (jnp.maximum(jnp.where(at_ref[0] < d, y - 1, y), 0), 0, 0, 0)

        return pl.BlockSpec((1, 4, 128, width), index)

    work = 16 * heads * 128 * 9 * 256 * 2 * 512
    return pl.pallas_call(
        lambda *r: attn_kernel(heads, *r),
        out_shape=jax.ShapeDtypeStruct((32, 4, 16, heads * 128), jnp.bfloat16),
        grid_spec=pltpu.PrefetchScalarGridSpec(
            num_scalar_prefetch=3,
            grid=(4,),
            in_specs=[
                pl.BlockSpec((1, 4, 128, heads * 128), lambda y, *_: (y, 0, 0, 0)),
            ] + [back(4, 128), back(4, 128), back(3, 256), back(2, 256), back(1, 256), back(0, 256)],
            out_specs=pl.BlockSpec((32, 1, 16, heads * 128), lambda y, *_: (0, y, 0, 0)),
            scratch_shapes=[
                pltpu.VMEM((REACH + BLOCK, 256), jnp.bfloat16),
                pltpu.VMEM((144, REACH + BLOCK), jnp.bfloat16),
                pltpu.VMEM((heads * TILE, 256), jnp.bfloat16),
                pltpu.SMEM((32,), jnp.int32),
            ],
        ),
        compiler_params=pltpu.CompilerParams(vmem_limit_bytes=VM << 20),
        cost_estimate=pl.CostEstimate(flops=work, bytes_accessed=16 << 20, transcendentals=0),
        name="attend",
    )(docs, plan, at, q, *kv)


VM = 52


AXES = ("y", "z", "core", "x")
SIZES = (4, 4)
FIRST = (0, 4)


def pack_kernel(seat, tab, keys, values, out):
    cos, sin = tables(tab, seat[0])
    for g in range(8):
        k = rotated(keys[:, g * 128:g * 128 + 128], cos, sin)
        v = values[:, g * 128:g * 128 + 128].T
        for twin in range(2):
            out[2 * g + twin, :, 0:128] = k
            out[2 * g + twin, :, 128:256] = v


def pack(seat, tab, keys, values):
    return pl.pallas_call(
        pack_kernel,
        out_shape=jax.ShapeDtypeStruct((16, 128, 256), jnp.bfloat16),
        in_specs=[pl.BlockSpec(memory_space=pltpu.SMEM)] + [pl.BlockSpec(memory_space=pltpu.VMEM)] * 3,
        name="pack",
    )(seat, tab, keys, values)


def split_kernel(seat, tab, rows, *outs):
    cos, sin = tables(tab, seat[0])
    for g in range(4):
        for first, size, out in zip(FIRST, SIZES, outs):
            for h in range(size):
                col = g * 1024 + (first + h) * 128
                out[g, :, h * 128:h * 128 + 128] = rotated(rows[:, col:col + 128], cos, sin)


def split(seat, tab, rows):
    return pl.pallas_call(
        split_kernel,
        grid=(4,),
        out_shape=[jax.ShapeDtypeStruct((16, 128, n * 128), jnp.bfloat16) for n in SIZES],
        in_specs=[
            pl.BlockSpec(memory_space=pltpu.SMEM),
            pl.BlockSpec((512, 128), lambda g: (0, 0)),
            pl.BlockSpec((128, 4096), lambda g: (0, g)),
        ],
        out_specs=[pl.BlockSpec((4, 128, n * 128), lambda g: (g, 0, 0)) for n in SIZES],
        cost_estimate=pl.CostEstimate(flops=2 << 30, bytes_accessed=8 << 20, transcendentals=0),
        name="split",
    )(seat, tab, rows)


def place_kernel(first, size, part, *refs):
    out, buf, sem = refs[-3:]
    step = pl.program_id(0)

    def copy(y, x):
        cols = pl.ds(pl.multiple_of((y * 4 + x) * 1024 + first * 128, 128), size * 128)
        return pltpu.make_async_copy(buf.at[y, x], out.at[:, cols], sem.at[y, x])

    for x in range(4):
        for b in range(8):
            buf[step, x, b * 16:b * 16 + 16, :] = part[0, b, x]
        copy(step, x).start()

    @pl.when(step == 3)
    def _():
        for y in range(4):
            for x in range(4):
                copy(y, x).wait()


def place_last_kernel(first, size, part, rows, out, land, buf, got, sem):
    fetches = [pltpu.make_async_copy(part.at[y], land.at[y], got.at[y]) for y in range(4)]
    for fetch in fetches:
        fetch.start()
    copies = []
    for y in range(4):
        fetches[y].wait()
        for x in range(4):
            for b in range(8):
                buf[y, x, b * 16:b * 16 + 16, :] = land[y, b, x]
            cols = pl.ds((y * 4 + x) * 1024 + first * 128, size * 128)
            copies.append(pltpu.make_async_copy(buf.at[y, x], out.at[:, cols], sem.at[y, x]))
            copies[-1].start()
    for c in copies:
        c.wait()


def place_last(first, size, part, rows):
    return pl.pallas_call(
        functools.partial(place_last_kernel, first, size),
        out_shape=jax.ShapeDtypeStruct((128, 16384), jnp.bfloat16),
        in_specs=[pl.BlockSpec(memory_space=pltpu.HBM), pl.BlockSpec(memory_space=pl.ANY)],
        out_specs=pl.BlockSpec(memory_space=pl.ANY),
        scratch_shapes=[
            pltpu.VMEM((4, 8, 4, 16, size * 128), jnp.bfloat16),
            pltpu.VMEM((4, 4, 128, size * 128), jnp.bfloat16),
            pltpu.SemaphoreType.DMA((4,)),
            pltpu.SemaphoreType.DMA((4, 4)),
        ],
        input_output_aliases={1: 0},
        compiler_params=pltpu.CompilerParams(vmem_limit_bytes=12 << 20),
        cost_estimate=pl.CostEstimate(flops=1 << 30, bytes_accessed=4 << 20, transcendentals=0),
        name="place",
    )(part, rows)


def place(first, size, part, rows):
    before = [] if rows is None else [rows]
    return pl.pallas_call(
        functools.partial(place_kernel, first, size),
        grid=(4,),
        out_shape=jax.ShapeDtypeStruct((128, 16384), jnp.bfloat16),
        in_specs=[pl.BlockSpec((1, 8, 4, 16, size * 128), lambda y: (y, 0, 0, 0, 0))]
        + [pl.BlockSpec(memory_space=pl.ANY)] * len(before),
        out_specs=pl.BlockSpec(memory_space=pl.ANY),
        scratch_shapes=[
            pltpu.VMEM((4, 4, 128, size * 128), jnp.bfloat16),
            pltpu.SemaphoreType.DMA((4, 4)),
        ],
        input_output_aliases={1: 0} if before else {},
        compiler_params=pltpu.CompilerParams(vmem_limit_bytes=12 << 20),
        cost_estimate=pl.CostEstimate(flops=1 << 30, bytes_accessed=4 << 20, transcendentals=0),
        name="place",
    )(part, *before)


def ring(a, by):
    return lax.ppermute(a, "z", [(i, (i + by) % 4) for i in range(4)])


def swap(a):
    return lax.ppermute(a, "core", [(0, 1), (1, 0)])


def on_device(query_rows, token_keys, token_values, doc_lengths, block_plan):
    at = (lax.axis_index("z") * 2 + lax.axis_index("core")).astype(jnp.int32).reshape(1)
    core = lax.axis_index("core")
    seat = ((lax.axis_index("y") * 8 + at[0]) * 4 + lax.axis_index("x")).astype(jnp.int32).reshape(1)
    tab = jnp.asarray(rotation_tables())
    kv = pack(seat, tab, token_keys, token_values)
    own = lax.all_to_all(kv, ("y", "x"), split_axis=0, concat_axis=0, tiled=True).reshape(4, 4, 128, 256)
    parts = split(seat, tab, query_rows)
    own, *parts = lax.optimization_barrier((own, *parts))
    near = ring(own, 1)
    left_values = ring(own[..., 128:], -1)
    far_keys = ring(near[..., :128], 1)
    far_values = ring(left_values, -1)
    first = swap(jnp.where(core == 0, own, near))
    parts[0] = lax.all_to_all(parts[0], ("y", "x"), split_axis=0, concat_axis=0, tiled=True)
    parts[0], middle = lax.optimization_barrier((parts[0], near))
    third = jnp.where(core == 0, middle, jnp.concatenate([far_keys, far_values], axis=-1))
    third = swap(third)
    kv = (far_keys, far_values, third, near, first, own)
    rows = None
    for j, (size, part) in enumerate(zip(SIZES, parts)):
        if j > 0:
            part = lax.all_to_all(part, ("y", "x"), split_axis=0, concat_axis=0, tiled=True)
        o = attend(size, doc_lengths, block_plan, at, part.reshape(4, 4, 128, size * 128), kv)
        o = lax.all_to_all(o.reshape(128, 16, size * 128), AXES, split_axis=0, concat_axis=0, tiled=True)
        put = place if rows is None else place_last
        rows = put(FIRST[j], size, o.reshape(4, 8, 4, 16, size * 128), rows)
    return rows


def solution(mesh):
    fine = jax.sharding.Mesh(mesh.devices.reshape(4, 4, 2, 4), AXES)
    rows = P(AXES, None)

    return jax.shard_map(on_device, mesh=fine, in_specs=(rows, rows, rows, P(), P()), out_specs=rows, check_vma=False)
```
